256 devices in a mesh: round: 2 (over x_hi), seq: 128 (over z, x_lo, y, core).
Axes of the slice: x: 4 (x_hi: 2, x_lo: 2; x = x_hi * 2 + x_lo), y: 4, z: 8, core: 2. Of those that a mesh axis runs over, the one named last changes fastest.
Arguments:
- qk: bfloat16 [65536, 1024], P('seq'), may hold values from -96 to 96
- values: bfloat16 [65536, 1024], P('seq'), may hold values from -6 to 6
- dest_dev: int32 [2, 65536], P('round', 'seq'), may hold values from 0 to 127, as said below
- dest_slot: int32 [2, 65536], P('round', 'seq'), may hold values from 0 to 511, as said below
Outputs:
- merged: bfloat16 [65536, 1024], P('seq', 'round')
The draws below stay inside these ranges and needn't reach their ends.
Inputs may be any that keep to these rules, and one draw needn't show every extreme that they name: dest_dev and dest_slot together send each round's 65536 tokens to 65536 distinct positions. In each round, from the rows of one index of seq at most 6 go to any one index of seq, and exactly 6 for some pair; every index receives exactly 512 rows. `dest_slot`: the row within the destination's block, see dest_dev.
All inputs are finite; a program needn't handle non-finite values.
Results may differ from the reference program's by a relative error of at most 0.03.
Values may be sent and summed in bfloat16 or wider, within the bound.
No kernel may reach another device: no remote copies, remote signals or barrier semaphores. Data moves between devices by JAX's collectives and lax.ppermute only.
A program may use at most 64 MiB of HBM per device.

```python
import jax
import jax.numpy as jnp
from jax import lax

D = 1024
HEADS = 8
HEAD_DIM = 128
STRETCH = 512
TOK_DEV = 512
ROUNDS = 2
TOKENS = 65536
HALF = 2
N_SEQ = 128


def route_round(key):
    shards = N_SEQ
    keys = jax.random.split(key, 6)
    lifts = jax.random.randint(keys[0], (shards // 2,), 0, HALF + 1)
    lifts = lifts.at[0].set(HALF)
    offsets = jnp.concatenate([lifts, -lifts])[jax.random.permutation(keys[1], shards)]
    sigma = jax.random.permutation(keys[2], shards)
    shuffle = jax.random.permutation(keys[3], shards)
    counts = 2 * HALF + offsets[(shuffle[None, :] - sigma[:, None]) % shards]
    ends = jnp.cumsum(counts, axis=1)
    starts = ends - counts
    spots = jnp.arange(TOK_DEV, dtype=jnp.int32)
    target = jnp.sum((spots[None, :, None] >= ends[:, None, :]).astype(jnp.int32), axis=2)
    ranks = spots[None, :] - jnp.take_along_axis(starts, target, axis=1)
    incoming = jnp.cumsum(counts, axis=0) - counts
    arrival = jnp.take_along_axis(incoming, target, axis=1) + ranks
    slot_orders = jax.vmap(lambda k: jax.random.permutation(k, TOK_DEV))(jax.random.split(keys[4], shards))
    slots = slot_orders[target, arrival]
    row_orders = jax.vmap(lambda k: jax.random.permutation(k, TOK_DEV))(jax.random.split(keys[5], shards))
    sources = jnp.arange(shards, dtype=jnp.int32)[:, None]
    dests = jnp.zeros((shards, TOK_DEV), jnp.int32).at[sources, row_orders].set(target.astype(jnp.int32))
    places = jnp.zeros((shards, TOK_DEV), jnp.int32).at[sources, row_orders].set(slots.astype(jnp.int32))
    return (dests.reshape(-1), places.reshape(-1))


def routing(key):
    base = jax.random.fold_in(key, 7001)
    return jax.vmap(route_round)(jax.random.split(base, ROUNDS))


def draw_dest_dev(key, part):
    return routing(key)[0]


def draw_dest_slot(key, part):
    return routing(key)[1]


def draw_qk(key, part):
    noise_key = jax.random.fold_in(key, 11)
    field = jax.random.truncated_normal(noise_key, -6.0, 6.0, (TOKENS, D))
    return field.astype(jnp.bfloat16)


def block_scale(key, shape, pieces, smallest, high):
    def one(axis_at, shards_of):
        steps = jax.random.uniform(jax.random.fold_in(jax.random.fold_in(key, 6), axis_at), (shards_of,), jnp.float32, smallest / len(pieces), high / len(pieces))
        return jnp.repeat(jnp.exp(steps), shape[axis_at] // shards_of).reshape((-1,) + (1,) * (len(shape) - axis_at - 1))

    gain = one(*pieces[0])
    for cut in pieces[1:]:
        gain = gain * one(*cut)
    return gain


def normal_values(stream_key, shape, spread, bound, cuts=(), held_as=jnp.bfloat16):
    array = spread * jax.random.normal(stream_key, shape, jnp.float32)
    if cuts:
        array = array * block_scale(stream_key, shape, cuts, -0.22, 0.18)
    return jnp.clip(array, -bound, bound).astype(held_as)


def setup_inputs(seed: int = 0) -> dict:
    arg_keys = jax.random.split(jax.random.key(seed), 5)
    qk = draw_qk(jax.random.fold_in(arg_keys[4], 71), 0)
    values = normal_values(arg_keys[1], (TOKENS, D), 1.0, 6.0, ((0, 128),))
    dest_dev = draw_dest_dev(jax.random.fold_in(arg_keys[4], 71), 0)
    dest_slot = draw_dest_slot(jax.random.fold_in(arg_keys[4], 71), 0)
    return dict(qk=qk, values=values, dest_dev=dest_dev, dest_slot=dest_slot)


eps_norm = 1e-06
self_score = -100000.0

def unit_keys(rows):
    count = rows.shape[0]
    heads = rows.shape[1] // HEAD_DIM
    field = rows.astype(jnp.float32).reshape(count, heads, HEAD_DIM)
    field = field * lax.rsqrt(lax.optimization_barrier(jnp.sum(field * field, axis=-1, keepdims=True)) + eps_norm)
    return field.reshape(count, heads * HEAD_DIM).astype(jnp.bfloat16)

def window_attend(queries, keys, vals):
    rows = queries.shape[0]
    heads = queries.shape[1] // HEAD_DIM
    qcast = queries.astype(jnp.float32).reshape(rows, heads, HEAD_DIM)
    kcast = keys.astype(jnp.float32).reshape(2 * rows, heads, HEAD_DIM)
    vcast = vals.astype(jnp.float32).reshape(2 * rows, heads, HEAD_DIM)
    scores = jnp.einsum('qhd,khd->hqk', qcast, kcast)
    itself = jnp.arange(2 * rows, dtype=jnp.int32)[None, :] == jnp.arange(rows, dtype=jnp.int32)[:, None] + rows
    scores = jnp.where(itself[None], jnp.float32(self_score), scores)
    highest = lax.optimization_barrier(jnp.max(scores, axis=-1))
    lse = highest + jnp.log(lax.optimization_barrier(jnp.sum(jnp.exp(scores - highest[..., None]), axis=-1)))
    probs = jnp.exp(scores - lse[..., None]).astype(jnp.bfloat16)
    attended = jnp.einsum('hqk,khd->qhd', probs.astype(jnp.float32), vcast)
    return (attended.reshape(rows, heads * HEAD_DIM).astype(jnp.bfloat16), jnp.transpose(lse))

def reference(qk, values, dest_dev, dest_slot):
    count = TOKENS // STRETCH
    outs = []
    lses = []
    for index in range(ROUNDS):
        place = (dest_dev[index] * TOK_DEV + dest_slot[index]).astype(jnp.int32)
        inverse = jnp.zeros((TOKENS,), jnp.int32).at[place].set(jnp.arange(TOKENS, dtype=jnp.int32))
        sorted_qk = qk[inverse]
        sorted_values = values[inverse]
        keys = unit_keys(sorted_qk)
        ext_keys = jnp.concatenate([keys[-STRETCH:], keys], axis=0)
        ext_values = jnp.concatenate([sorted_values[-STRETCH:], sorted_values], axis=0)

        def one_stretch(position):
            start = (position * STRETCH).astype(jnp.int32)
            queries = lax.dynamic_slice_in_dim(sorted_qk, start, STRETCH, 0)
            window_keys = lax.dynamic_slice_in_dim(ext_keys, start, 2 * STRETCH, 0)
            window_values = lax.dynamic_slice_in_dim(ext_values, start, 2 * STRETCH, 0)
            return window_attend(queries, window_keys, window_values)
        attended, lse = lax.map(one_stretch, jnp.arange(count, dtype=jnp.int32))
        attended = attended.reshape(TOKENS, D)
        lse = lse.reshape(TOKENS, HEADS)
        outs.append(attended[place])
        lses.append(lse[place])
    stacked = jnp.stack(lses)
    highest = lax.optimization_barrier(jnp.max(stacked, axis=0))
    total = highest + jnp.log(lax.optimization_barrier(jnp.sum(jnp.exp(stacked - highest[None]), axis=0)))
    merged = jnp.zeros((TOKENS, D), jnp.float32)
    for index in range(ROUNDS):
        weight = jnp.repeat(jnp.exp(lses[index] - total), HEAD_DIM, axis=1)
        merged = merged + weight * outs[index].astype(jnp.float32)
    return merged.astype(jnp.bfloat16)
```

```python
import jax
import jax.numpy as jnp
from jax import lax
from jax.experimental import pallas as pl
from jax.experimental.pallas import tpu as pltpu
from jax.sharding import PartitionSpec as P

HEAD = 128
ROWS = 512
CAP = 6
HOPS = 4
PEERS = 32
STR = 4
PB = STR * CAP
MSG = HOPS * PB
TOT = PEERS * MSG
BLK = 384
LROWS = 16
QK_MAX = 96.0
PAD_MARK = 1024.0

eps_norm = 1e-06
self_score = -100000.0

bf16 = jnp.bfloat16
f32 = jnp.float32
i32 = jnp.int32


def iota(shape, dim):
    return lax.broadcasted_iota(i32, shape, dim)


def dot(a, b):
    return lax.dot_general(a, b, (((1,), (0,)), ((), ())), preferred_element_type=f32)


def dot_nt(a, b):
    return lax.dot_general(a, b, (((1,), (1,)), ((), ())), preferred_element_type=f32)


def ones_where(mask):
    return jnp.where(mask, 1.0, 0.0).astype(bf16)


def call(body, out_shape, scratch=(), **kw):
    return pl.pallas_call(
        body,
        out_shape=out_shape,
        scratch_shapes=list(scratch),
        compiler_params=pltpu.CompilerParams(vmem_limit_bytes=56 << 20),
        **kw,
    )


def split_body(group_ref, qk_ref, v_ref, o_ref):
    o_ref[0, :, 0:HEAD] = qk_ref[...]
    o_ref[0, :, HEAD:] = v_ref[...]


def split_heads(group, qk, values):
    return pl.pallas_call(
        split_body,
        out_shape=jax.ShapeDtypeStruct((HOPS, ROWS, 2 * HEAD), bf16),
        grid_spec=pltpu.PrefetchScalarGridSpec(
            num_scalar_prefetch=1,
            grid=(HOPS,),
            in_specs=[
                pl.BlockSpec((ROWS, HEAD), lambda k, g: (0, g[0] * HOPS + k)),
                pl.BlockSpec((ROWS, HEAD), lambda k, g: (0, g[0] * HOPS + k)),
            ],
            out_specs=pl.BlockSpec((1, ROWS, 2 * HEAD), lambda k, g: (k, 0, 0)),
        ),
        name="split_heads",
    )(group, qk, values)


def place_body(col_ref, row_ref, o_ref):
    same = col_ref[...] == row_ref[...]
    before = iota((ROWS, ROWS), 0) < iota((ROWS, ROWS), 1)
    hits = jnp.where(same & before, 1.0, 0.0)
    rank = jnp.sum(hits, axis=0, keepdims=True).astype(i32)
    o_ref[...] = row_ref[...] * CAP + rank


def places(dest):
    return call(place_body, jax.ShapeDtypeStruct((1, ROWS), i32), name="places")(
        dest.reshape(ROWS, 1), dest.reshape(1, ROWS)
    )


def pack_body(pos_ref, x_ref, o_ref, acc_ref):
    slots = PEERS * PB
    ids = iota((slots, ROWS), 0)
    ones = jnp.full((ROWS, HEAD), 1.0, bf16)
    for j in range(HOPS):
        pick = ones_where(pos_ref[j : j + 1, :] == ids)
        got = dot(pick, x_ref[j])
        mark = (1.0 - dot(pick, ones)) * PAD_MARK
        lo, hi = j * PB, (j + 1) * PB
        acc_ref[:, lo:hi, 0:HEAD] = (got[:, 0:HEAD] + mark).reshape(PEERS, PB, HEAD)
        acc_ref[:, lo:hi, HEAD:] = got[:, HEAD:].reshape(PEERS, PB, HEAD)
    o_ref[...] = acc_ref[...].astype(bf16)


def pack(pos, x):
    shape = (PEERS, MSG, 2 * HEAD)
    return call(
        pack_body,
        jax.ShapeDtypeStruct(shape, bf16),
        [pltpu.VMEM(shape, f32)],
        name="pack",
    )(pos, x)


def stretch_of(ids):
    return ((ids * 10923) >> 16) & (STR - 1)


def compact_body(x_ref, o_ref, tail_ref, tcol_ref, trow_ref):
    rq = stretch_of(iota((1, BLK), 1))
    cq = stretch_of(iota((BLK, 1), 0))
    same = rq == cq
    row_id, col_id = iota((BLK, BLK), 0), iota((BLK, BLK), 1)
    lower = ones_where(same & (col_id < row_id))
    upper = ones_where(same & (row_id < col_id))
    both = ones_where(same)
    first = ones_where((iota((8, HEAD), 1) == 0))
    base_col = jnp.broadcast_to(cq, (BLK, HEAD)).astype(f32) * float(ROWS)
    base_row = jnp.broadcast_to(rq, (8, BLK)).astype(f32) * float(ROWS)
    for k in range(TOT // BLK):
        x = x_ref[k * BLK : (k + 1) * BLK, 0:HEAD]
        lead = jnp.broadcast_to(x.astype(f32)[:, 0:1], (BLK, HEAD))
        ok = jnp.abs(lead) <= QK_MAX
        okb = ones_where(ok)
        tcol_ref[k * BLK : (k + 1) * BLK, :] = jnp.where(ok, base_col + dot(lower, okb), -1.0)
        base_col = base_col + dot(both, okb)
        rok = jnp.abs(dot_nt(first, x)) <= QK_MAX
        rokb = ones_where(rok)
        trow = jnp.where(rok, base_row + dot(rokb, upper), -1.0)
        trow_ref[:, k * BLK : (k + 1) * BLK] = trow.astype(i32)
        base_row = base_row + dot(rokb, both)
    for q in range(STR):
        pick = ones_where(trow_ref[0:1, :] == iota((ROWS, TOT), 0) + q * ROWS)
        got = dot(pick, x_ref[...]).astype(bf16)
        o_ref[q * ROWS : (q + 1) * ROWS, :] = got
        if q == STR - 1:
            tail_ref[...] = got


def compact(x):
    return call(
        compact_body,
        (
            jax.ShapeDtypeStruct((STR * ROWS, 2 * HEAD), bf16),
            jax.ShapeDtypeStruct((ROWS, 2 * HEAD), bf16),
            jax.ShapeDtypeStruct((TOT, HEAD), f32),
        ),
        [pltpu.VMEM((8, TOT), i32)],
        name="compact",
    )(x)


def unit(x):
    x = x.astype(f32)
    return (x * lax.rsqrt(jnp.sum(x * x, axis=1, keepdims=True) + eps_norm)).astype(bf16)


def attend_body(x_ref, halo_ref, tcol_ref, o_ref, res_ref, lse_ref):
    own = iota((ROWS, ROWS), 0) == iota((ROWS, ROWS), 1)
    lane = iota((ROWS, HEAD), 1)
    prev_k = unit(halo_ref[:, 0:HEAD])
    prev_v = halo_ref[:, HEAD:]
    for q in range(STR):
        rows = slice(q * ROWS, (q + 1) * ROWS)
        qs = x_ref[rows, 0:HEAD]
        vs = x_ref[rows, HEAD:]
        ks = unit(qs)
        sa = dot_nt(qs, prev_k)
        sb = jnp.where(own, self_score, dot_nt(qs, ks))
        top = jnp.maximum(
            jnp.max(sa, axis=1, keepdims=True), jnp.max(sb, axis=1, keepdims=True)
        )
        pa = jnp.exp(sa - top)
        pb = jnp.exp(sb - top)
        total = jnp.sum(pa, axis=1, keepdims=True) + jnp.sum(pb, axis=1, keepdims=True)
        out = dot(pa.astype(bf16), prev_v) + dot(pb.astype(bf16), vs)
        lse = top + jnp.log(total)
        high = lse.astype(bf16).astype(f32)
        low = lse - high
        res_ref[rows, 0:HEAD] = (out / total).astype(bf16)
        res_ref[rows, HEAD:] = jnp.where(
            lane == 0, high, jnp.where(lane == 1, low, 0.0)
        ).astype(bf16)
        prev_k, prev_v = ks, vs
    lse_ref[TOT:, :] = jnp.zeros((HEAD, HEAD), bf16)
    cols = iota((BLK, STR * ROWS), 1)
    for k in range(TOT // BLK):
        spots = tcol_ref[k * BLK : (k + 1) * BLK, 0:1].astype(i32)
        got = dot(ones_where(spots == cols), res_ref[...]).astype(bf16)
        for i in range(BLK // MSG):
            o_ref[k * (BLK // MSG) + i, 0:MSG, :] = got[i * MSG : (i + 1) * MSG, 0:HEAD]
        lse_ref[k * BLK : (k + 1) * BLK, :] = got[:, HEAD:]
    eye = ones_where(iota((LROWS, HEAD), 0) == iota((LROWS, HEAD), 1))
    for p in range(PEERS):
        o_ref[p, MSG:, :] = dot_nt(eye, lse_ref[p * MSG : p * MSG + HEAD, :]).astype(bf16)


def attend(x, halo, tcol):
    return call(
        attend_body,
        jax.ShapeDtypeStruct((PEERS, MSG + LROWS, HEAD), bf16),
        [pltpu.VMEM((STR * ROWS, 2 * HEAD), bf16), pltpu.VMEM((TOT + HEAD, HEAD), bf16)],
        name="attend",
    )(x, halo, tcol)


def merge_body(pos_ref, a_ref, b_ref, o_ref, acc_ref):
    slots = PEERS * PB
    pos = pos_ref[...]
    peer = (pos * 2731) >> 16
    hop = iota(pos.shape, 0) & (HOPS - 1)
    spot = pos - peer * PB + hop * PB
    cols = jnp.concatenate([pos, peer, spot], axis=0).astype(f32).T.astype(i32)
    lanes = iota((ROWS, slots), 1)
    spots = iota((ROWS, HEAD), 1)
    peers = iota((ROWS, PEERS * LROWS), 1) >> 4
    outs, lses = [], []
    for r, ref in enumerate((a_ref, b_ref)):
        acc_ref[...] = ref[...].astype(f32)
        packed = ref[:, MSG:, :].reshape(PEERS * LROWS, HEAD)
        for j in range(HOPS):
            c = r * HOPS + j
            rows = acc_ref[:, j * PB : (j + 1) * PB, :].reshape(slots, HEAD).astype(bf16)
            outs.append(dot(ones_where(cols[:, c : c + 1] == lanes), rows))
            near = dot_nt(ones_where(cols[:, 16 + c : 17 + c] == spots), packed)
            mine = cols[:, 8 + c : 9 + c] == peers
            lses.append(jnp.sum(jnp.where(mine, near, 0.0), axis=1, keepdims=True))
    for j in range(HOPS):
        la, lb = lses[j], lses[HOPS + j]
        top = jnp.maximum(la, lb)
        ea, eb = jnp.exp(la - top), jnp.exp(lb - top)
        o_ref[j] = ((ea * outs[j] + eb * outs[HOPS + j]) / (ea + eb)).astype(bf16)


def merge(pos, a, b):
    return call(
        merge_body,
        jax.ShapeDtypeStruct((HOPS, ROWS, HEAD), bf16),
        [pltpu.VMEM((PEERS, MSG + LROWS, HEAD), f32)],
        name="merge",
    )(pos, a, b)


def join_body(x_ref, o_ref):
    o_ref[...] = x_ref[0]


def join_heads(x):
    return pl.pallas_call(
        join_body,
        out_shape=jax.ShapeDtypeStruct((ROWS, HOPS * HEAD), bf16),
        grid=(HOPS,),
        in_specs=[pl.BlockSpec((1, ROWS, HEAD), lambda k: (k, 0, 0))],
        out_specs=pl.BlockSpec((ROWS, HEAD), lambda k: (0, k)),
        name="join_heads",
    )(x)


FAR = [[PEERS * j + p for j in range(HOPS)] for p in range(PEERS)]
NEAR = [[PEERS * j + p for p in range(PEERS)] for j in range(HOPS)]
NEXT = [(PEERS * j + p, PEERS * j + (p + 1) % PEERS) for j in range(HOPS) for p in range(PEERS)]


def swap(x, groups):
    return lax.all_to_all(x, "seq", 0, 0, tiled=True, axis_index_groups=groups)


def on_device(qk, values, dest_dev, dest_slot):
    group = lax.axis_index("round").astype(i32).reshape(1)
    mine = swap(split_heads(group, qk, values), FAR)
    pos = places(dest_dev[0])
    pos = lax.all_gather(pos, "round", axis=0, tiled=True)
    pos = lax.all_gather(pos, "seq", axis=1, axis_index_groups=FAR)
    pos = pos.reshape(2 * HOPS, ROWS)
    replies = []
    for r in range(2):
        sent = pack(pos[r * HOPS : (r + 1) * HOPS], mine)
        got = swap(sent, NEAR)
        rows, tail, tcol = compact(got.reshape(TOT, 2 * HEAD))
        halo = lax.ppermute(tail, "seq", NEXT)
        replies.append(swap(attend(rows, halo, tcol), NEAR))
    merged = merge(pos, *replies)
    return join_heads(swap(merged, FAR))


def solution(mesh):
    return jax.shard_map(
        on_device,
        mesh=mesh,
        in_specs=(P("seq", None), P("seq", None), P("round", "seq"), P("round", "seq")),
        out_specs=P("seq", "round"),
        check_vma=False,
    )
```

```python
import jax
import jax.numpy as jnp
from jax import lax
from jax.experimental import pallas as pl
from jax.experimental.pallas import tpu as pltpu
from jax.sharding import PartitionSpec as P

HEAD = 128
ROWS = 512
CAP = 6
UNIT = 8
HOPS = 4
PEERS = 32
STR = 4
PB = HOPS * CAP
MSG = STR * PB
SLOTS = PEERS * PB
PLACES = PEERS * STR * UNIT
EXTRA = 16
QK_MAX = 96.0
PAD_MARK = 1024.0

eps_norm = 1e-06
self_score = -100000.0

bf16 = jnp.bfloat16
f32 = jnp.float32
i32 = jnp.int32


def iota(shape, dim):
    return lax.broadcasted_iota(i32, shape, dim)


def dot(a, b):
    return lax.dot_general(a, b, (((1,), (0,)), ((), ())), preferred_element_type=f32)


def dot_nt(a, b):
    return lax.dot_general(a, b, (((1,), (1,)), ((), ())), preferred_element_type=f32)


def ones_where(mask):
    return jnp.where(mask, 1.0, 0.0).astype(bf16)


def call(body, out_shape, scratch=(), **kw):
    return pl.pallas_call(
        body,
        out_shape=out_shape,
        scratch_shapes=list(scratch),
        compiler_params=pltpu.CompilerParams(vmem_limit_bytes=56 << 20),
        **kw,
    )


def place_rows(dest):
    col = jnp.broadcast_to(dest.astype(f32), (8, ROWS)).T[:, 0:1]
    same = col == dest.astype(f32)
    before = iota((ROWS, ROWS), 0) < iota((ROWS, ROWS), 1)
    rank = jnp.sum(jnp.where(same & before, 1.0, 0.0), axis=0, keepdims=True)
    pos = dest * UNIT + rank.astype(i32)
    high = pos >> 4
    low = pos - high * 16
    half = ROWS // 2
    parts = [x[:, h * half : (h + 1) * half] for h in range(2) for x in (high, low)]
    return jnp.concatenate(parts, axis=0).astype(f32)


def split_body(group_ref, own_ref, other_ref, qk_ref, v_ref, o_ref, sems):
    start = pl.multiple_of(group_ref[0] * (HOPS * HEAD), HEAD)
    copies = []
    for k in range(HOPS):
        for n, ref in enumerate((qk_ref, v_ref)):
            copies.append(
                pltpu.make_async_copy(
                    ref.at[:, pl.ds(start + k * HEAD, HEAD)],
                    o_ref.at[k, 0:ROWS, n * HEAD : (n + 1) * HEAD],
                    sems.at[k * 2 + n],
                )
            )
    for c in copies:
        c.start()
    own = place_rows(own_ref[...])
    other = place_rows(other_ref[...])
    mine = group_ref[0] == 0
    rows = jnp.concatenate(
        [jnp.where(mine, own, other), jnp.where(mine, other, own), jnp.zeros((8, ROWS // 2), f32)],
        axis=0,
    ).astype(bf16)
    for k in range(HOPS):
        o_ref[k, ROWS:, :] = rows
    for c in copies:
        c.wait()


def split_heads(group, own, other, qk, values):
    vmem = pl.BlockSpec(memory_space=pltpu.VMEM)
    hbm = pl.BlockSpec(memory_space=pl.ANY)
    return call(
        split_body,
        jax.ShapeDtypeStruct((HOPS, ROWS + EXTRA, 2 * HEAD), bf16),
        [pltpu.SemaphoreType.DMA((2 * HOPS,))],
        in_specs=[pl.BlockSpec(memory_space=pltpu.SMEM), vmem, vmem, hbm, hbm],
        name="split_heads",
    )(group, own, other, qk, values)


def pack(x, r):
    def body(x_ref, o_ref, pos_ref, acc_ref):
        ids = iota((PLACES, ROWS), 0)
        ones = jnp.full((ROWS, HEAD), 1.0, bf16)
        for j in range(HOPS):
            rows = x_ref[j, ROWS:, :].astype(f32)[4 * r : 4 * r + 4]
            pos = jnp.concatenate(
                [rows[0:1] * 16.0 + rows[1:2], rows[2:3] * 16.0 + rows[3:4]], axis=1
            ).astype(i32)
            pos_ref[j : j + 1, :] = pos
            pick = ones_where(pos == ids)
            got = dot(pick, x_ref[j, 0:ROWS, :])
            mark = (1.0 - dot(pick, ones)) * PAD_MARK
            left = (got[:, 0:HEAD] + mark).reshape(PEERS, STR, UNIT, HEAD)
            right = got[:, HEAD:].reshape(PEERS, STR, UNIT, HEAD)
            for q in range(STR):
                at = q * PB + j * CAP
                acc_ref[:, at : at + CAP, 0:HEAD] = left[:, q, 0:CAP, :]
                acc_ref[:, at : at + CAP, HEAD:] = right[:, q, 0:CAP, :]
        o_ref[...] = acc_ref[...].astype(bf16)

    shape = (PEERS, MSG, 2 * HEAD)
    return call(
        body,
        (jax.ShapeDtypeStruct(shape, bf16), jax.ShapeDtypeStruct((HOPS, ROWS), i32)),
        [pltpu.VMEM(shape, f32)],
        name="pack",
    )(x)


def compact_body(x_ref, o_ref, tail_ref, tcol_ref):
    lower = ones_where(iota((SLOTS, SLOTS), 1) < iota((SLOTS, SLOTS), 0))
    first = ones_where(iota((8, HEAD), 1) == 0)
    lane = iota((SLOTS, HEAD), 1)
    sub = iota((8, SLOTS), 0)
    row_ok = jnp.zeros((8, SLOTS), f32)
    col_ok = jnp.zeros((SLOTS, HEAD), f32)
    parts = []
    for pair in range(STR // 2):
        both = x_ref[:, pair * 2 * PB : (pair + 1) * 2 * PB, :].astype(f32)
        for half in range(2):
            q = pair * 2 + half
            x = both[:, half * PB : (half + 1) * PB, :].reshape(SLOTS, 2 * HEAD)
            lead = jnp.broadcast_to(x[:, 0:1], (SLOTS, HEAD))
            col_ok = jnp.where((lane == q) & (jnp.abs(lead) <= QK_MAX), 1.0, col_ok)
            x = x.astype(bf16)
            ahead = dot_nt(first, x[:, 0:HEAD])
            row_ok = jnp.where((sub == q) & (jnp.abs(ahead) <= QK_MAX), 1.0, row_ok)
            parts.append(x)
    tcol_ref[...] = jnp.where(col_ok > 0.0, dot(lower, col_ok.astype(bf16)), -1.0)
    trow = jnp.where(row_ok > 0.0, dot_nt(row_ok.astype(bf16), lower), -1.0).astype(i32)
    ids = iota((ROWS, SLOTS), 0)
    for q in range(STR):
        got = dot(ones_where(trow[q : q + 1, :] == ids), parts[q]).astype(bf16)
        o_ref[q * ROWS : (q + 1) * ROWS, :] = got
        if q == STR - 1:
            tail_ref[...] = got


def compact(x):
    return call(
        compact_body,
        (
            jax.ShapeDtypeStruct((STR * ROWS, 2 * HEAD), bf16),
            jax.ShapeDtypeStruct((ROWS, 2 * HEAD), bf16),
            jax.ShapeDtypeStruct((SLOTS, HEAD), f32),
        ),
        name="compact",
    )(x)


def unit(x):
    x = x.astype(f32)
    return (x * lax.rsqrt(jnp.sum(x * x, axis=1, keepdims=True) + eps_norm)).astype(bf16)


def attend_body(x_ref, halo_ref, tcol_ref, o_ref, out_ref, lse_ref):
    own = iota((ROWS, ROWS), 0) == iota((ROWS, ROWS), 1)
    lane = iota((ROWS, HEAD), 1)
    cols = iota((SLOTS, ROWS), 1)
    lse_ref[:, MSG:, :] = jnp.zeros((PEERS, HEAD - MSG, HEAD), f32)
    prev_k = unit(halo_ref[:, 0:HEAD])
    prev_v = halo_ref[:, HEAD:]
    for q in range(STR):
        rows = slice(q * ROWS, (q + 1) * ROWS)
        qs = x_ref[rows, 0:HEAD]
        vs = x_ref[rows, HEAD:]
        ks = unit(qs)
        sa = dot_nt(qs, prev_k)
        sb = jnp.where(own, self_score, dot_nt(qs, ks))
        top = jnp.maximum(
            jnp.max(sa, axis=1, keepdims=True), jnp.max(sb, axis=1, keepdims=True)
        )
        pa = jnp.exp(sa - top)
        pb = jnp.exp(sb - top)
        total = jnp.sum(pa, axis=1, keepdims=True) + jnp.sum(pb, axis=1, keepdims=True)
        out = dot(pa.astype(bf16), prev_v) + dot(pb.astype(bf16), vs)
        lse = top + jnp.log(total)
        high = lse.astype(bf16).astype(f32)
        low = lse - high
        side = jnp.where(lane == 0, high, jnp.where(lane == 1, low, 0.0))
        res = jnp.concatenate([(out / total).astype(bf16), side.astype(bf16)], axis=1)
        pick = ones_where(tcol_ref[:, q : q + 1].astype(i32) == cols)
        got = dot(pick, res)
        at = q * PB
        out_ref[:, at : at + PB, :] = got[:, 0:HEAD].reshape(PEERS, PB, HEAD)
        lse_ref[:, at : at + PB, :] = got[:, HEAD:].reshape(PEERS, PB, HEAD)
        prev_k, prev_v = ks, vs
    o_ref[:, 0:MSG, :] = out_ref[...].astype(bf16)
    eye = ones_where(iota((EXTRA, HEAD), 0) == iota((EXTRA, HEAD), 1))
    for p in range(PEERS):
        o_ref[p, MSG:, :] = dot_nt(eye, lse_ref[p].astype(bf16)).astype(bf16)


def attend(x, halo, tcol):
    return call(
        attend_body,
        jax.ShapeDtypeStruct((PEERS, MSG + EXTRA, HEAD), bf16),
        [pltpu.VMEM((PEERS, MSG, HEAD), f32), pltpu.VMEM((PEERS, HEAD, HEAD), f32)],
        name="attend",
    )(x, halo, tcol)


def unpacked(pos, x_ref, acc_ref):
    acc_ref[...] = x_ref[...].astype(f32)
    packed = x_ref[:, MSG:, :].reshape(PEERS * EXTRA, HEAD)
    peer = pos >> 5
    rest = pos - (peer << 5)
    quarter = rest >> 3
    spot = quarter * PB + iota(pos.shape, 0) * CAP + rest - (quarter << 3)
    cols = jnp.concatenate([pos, peer, spot, spot], axis=0).astype(f32).T.astype(i32)
    lanes = iota((ROWS, PLACES), 1)
    spots = iota((ROWS, HEAD), 1)
    peers = iota((ROWS, PEERS * EXTRA), 1) >> 4
    outs, lses = [], []
    for j in range(HOPS):
        pieces = [
            acc_ref[:, q * PB + j * CAP : q * PB + j * CAP + UNIT, :].reshape(PEERS, 1, UNIT, HEAD)
            for q in range(STR)
        ]
        rows = jnp.concatenate(pieces, axis=1).reshape(PLACES, HEAD).astype(bf16)
        outs.append(dot(ones_where(cols[:, j : j + 1] == lanes), rows))
        near = dot_nt(ones_where(cols[:, 8 + j : 9 + j] == spots), packed)
        mine = cols[:, 4 + j : 5 + j] == peers
        lses.append(jnp.sum(jnp.where(mine, near, 0.0), axis=1, keepdims=True))
    return outs, lses


def unpack_body(pos_ref, x_ref, o_ref, lse_ref, acc_ref):
    outs, lses = unpacked(pos_ref[...], x_ref, acc_ref)
    lane = iota((ROWS, HEAD), 1)
    side = jnp.zeros((ROWS, HEAD), f32)
    for j in range(HOPS):
        o_ref[j] = outs[j].astype(bf16)
        side = jnp.where(lane == j, lses[j], side)
    lse_ref[...] = side


ACC = (PEERS, MSG + EXTRA, HEAD)
HEADS_OUT = (HOPS, ROWS, HEAD)


def unpack(pos, x):
    return call(
        unpack_body,
        (jax.ShapeDtypeStruct(HEADS_OUT, bf16), jax.ShapeDtypeStruct((ROWS, HEAD), f32)),
        [pltpu.VMEM(ACC, f32)],
        name="unpack",
    )(pos, x)


def merge_body(pos_ref, x_ref, other_ref, other_lse_ref, o_ref, acc_ref):
    outs, lses = unpacked(pos_ref[...], x_ref, acc_ref)
    for j in range(HOPS):
        la, lb = other_lse_ref[:, j : j + 1], lses[j]
        top = jnp.maximum(la, lb)
        ea, eb = jnp.exp(la - top), jnp.exp(lb - top)
        o_ref[j] = ((ea * other_ref[j].astype(f32) + eb * outs[j]) / (ea + eb)).astype(bf16)


def merge(pos, x, other, other_lse):
    return call(
        merge_body,
        jax.ShapeDtypeStruct(HEADS_OUT, bf16),
        [pltpu.VMEM(ACC, f32)],
        name="merge",
    )(pos, x, other, other_lse)


def join_body(x_ref, o_ref):
    for k in range(HOPS):
        o_ref[:, k * HEAD : (k + 1) * HEAD] = x_ref[k]


def join_heads(x):
    return call(join_body, jax.ShapeDtypeStruct((ROWS, HOPS * HEAD), bf16), name="join_heads")(x)


FAR = [[PEERS * j + p for j in range(HOPS)] for p in range(PEERS)]
NEAR = [[PEERS * j + p for p in range(PEERS)] for j in range(HOPS)]
NEXT = [(PEERS * j + p, PEERS * j + (p + 1) % PEERS) for j in range(HOPS) for p in range(PEERS)]


def swap(x, groups):
    return lax.all_to_all(x, "seq", 0, 0, tiled=True, axis_index_groups=groups)


def on_device(qk, values, dest_dev, dest_slot):
    group = lax.axis_index("round").astype(i32).reshape(1)
    other = lax.ppermute(dest_dev, "round", [(0, 1), (1, 0)])
    mine = swap(split_heads(group, dest_dev, other, qk, values), FAR)
    spots, replies = [], []
    for r in range(2):
        sent, pos = pack(mine, r)
        rows, tail, tcol = compact(swap(sent, NEAR))
        halo = lax.ppermute(tail, "seq", NEXT)
        spots.append(pos)
        replies.append(swap(attend(rows, halo, tcol), NEAR))
    out, lse = unpack(spots[0], replies[0])
    return join_heads(swap(merge(spots[1], replies[1], out, lse), FAR))


def solution(mesh):
    return jax.shard_map(
        on_device,
        mesh=mesh,
        in_specs=(P("seq", None), P("seq", None), P("round", "seq"), P("round", "seq")),
        out_specs=P("seq", "round"),
        check_vma=False,
    )
```

```python
import jax
import jax.numpy as jnp
from jax import lax
from jax.experimental import pallas as pl
from jax.experimental.pallas import tpu as pltpu
from jax.sharding import PartitionSpec as P


HEAD = 128
ROWS = 512
CAP = 6
UNIT = 8
HOPS = 4
PEERS = 32
STR = 4
PB = HOPS * CAP
MSG = STR * PB
SLOTS = PEERS * PB
PLACES = PEERS * STR * UNIT
EXTRA = 16
QK_MAX = 96.0
PAD_MARK = 1024.0

eps_norm = 1e-06
self_score = -100000.0

bf16 = jnp.bfloat16
f32 = jnp.float32
i32 = jnp.int32


def iota(shape, dim):
    return lax.broadcasted_iota(i32, shape, dim)


def dot(a, b):
    return lax.dot_general(a, b, (((1,), (0,)), ((), ())), preferred_element_type=f32)


def dot_nt(a, b):
    return lax.dot_general(a, b, (((1,), (1,)), ((), ())), preferred_element_type=f32)


def ones_where(mask):
    return jnp.where(mask, 1.0, 0.0).astype(bf16)


def call(body, out_shape, scratch=(), **kw):
    return pl.pallas_call(
        body,
        out_shape=out_shape,
        scratch_shapes=list(scratch),
        compiler_params=pltpu.CompilerParams(vmem_limit_bytes=56 << 20),
        **kw,
    )


def place_rows(dest):
    col = jnp.broadcast_to(dest.astype(f32), (8, ROWS)).T[:, 0:1]
    same = col == dest.astype(f32)
    before = iota((ROWS, ROWS), 0) < iota((ROWS, ROWS), 1)
    rank = jnp.sum(jnp.where(same & before, 1.0, 0.0), axis=0, keepdims=True)
    pos = dest * UNIT + rank.astype(i32)
    high = pos >> 4
    low = pos - high * 16
    half = ROWS // 2
    parts = [x[:, h * half : (h + 1) * half] for h in range(2) for x in (high, low)]
    return jnp.concatenate(parts, axis=0).astype(f32)


def copy_all(copies):
    for c in copies:
        c.start()
    for c in copies:
        c.wait()


def lanes_of(spot):
    return pl.ds(pl.multiple_of(spot * HEAD, HEAD), HEAD)


def split_body(spot_ref, qk_ref, v_ref, *refs):
    outs, sems = refs[:HOPS], refs[HOPS]
    copies = []
    for o in range(HOPS):
        head = spot_ref[0] * HOPS + ((spot_ref[1] + o) & (HOPS - 1))
        for n, ref in enumerate((qk_ref, v_ref)):
            copies.append(
                pltpu.make_async_copy(
                    ref.at[:, lanes_of(head)],
                    outs[o].at[:, n * HEAD : (n + 1) * HEAD],
                    sems.at[o * 2 + n],
                )
            )
    copy_all(copies)


SMEM = pl.BlockSpec(memory_space=pltpu.SMEM)
HBM = pl.BlockSpec(memory_space=pl.ANY)


def split_heads(spot, qk, values):
    return call(
        split_body,
        (jax.ShapeDtypeStruct((ROWS, 2 * HEAD), bf16),) * HOPS,
        [pltpu.SemaphoreType.DMA((2 * HOPS,))],
        in_specs=[SMEM, HBM, HBM],
        name="split_heads",
    )(spot, qk, values)


def place_body(spot_ref, own_ref, other_ref, o_ref):
    own = place_rows(own_ref[...])
    other = place_rows(other_ref[...])
    mine = spot_ref[0] == 0
    o_ref[...] = jnp.concatenate(
        [jnp.where(mine, own, other), jnp.where(mine, other, own), jnp.zeros((8, ROWS // 2), f32)],
        axis=0,
    ).astype(bf16)


def places(spot, own, other):
    vmem = pl.BlockSpec(memory_space=pltpu.VMEM)
    return call(
        place_body,
        jax.ShapeDtypeStruct((EXTRA, 2 * HEAD), bf16),
        in_specs=[SMEM, vmem, vmem],
        name="places",
    )(spot, own, other)


def pack(xs, spots, r):
    def body(*refs):
        x_refs, e_refs = refs[:HOPS], refs[HOPS : 2 * HOPS]
        o_ref, pos_ref, acc_ref = refs[2 * HOPS :]
        ids = iota((PLACES, ROWS), 0)
        ones = jnp.full((ROWS, HEAD), 1.0, bf16)
        for j in range(HOPS):
            rows = e_refs[j][...].astype(f32)[4 * r : 4 * r + 4]
            pos = jnp.concatenate(
                [rows[0:1] * 16.0 + rows[1:2], rows[2:3] * 16.0 + rows[3:4]], axis=1
            ).astype(i32)
            pos_ref[j : j + 1, :] = pos
            pick = ones_where(pos == ids)
            got = dot(pick, x_refs[j][...])
            mark = (1.0 - dot(pick, ones)) * PAD_MARK
            left = (got[:, 0:HEAD] + mark).reshape(PEERS, STR, UNIT, HEAD)
            right = got[:, HEAD:].reshape(PEERS, STR, UNIT, HEAD)
            for q in range(STR):
                at = q * PB + j * CAP
                acc_ref[:, at : at + CAP, 0:HEAD] = left[:, q, 0:CAP, :]
                acc_ref[:, at : at + CAP, HEAD:] = right[:, q, 0:CAP, :]
        o_ref[...] = acc_ref[...].astype(bf16)

    shape = (PEERS, MSG, 2 * HEAD)
    return call(
        body,
        (jax.ShapeDtypeStruct(shape, bf16), jax.ShapeDtypeStruct((HOPS, ROWS), i32)),
        [pltpu.VMEM(shape, f32)],
        name="pack",
    )(*xs, *spots)


def tail_body(x_ref, o_ref):
    x = x_ref[...].astype(f32)[:, UNIT:, :].reshape(SLOTS, 2 * HEAD).astype(bf16)
    upper = ones_where(iota((SLOTS, SLOTS), 0) < iota((SLOTS, SLOTS), 1))
    first = ones_where(iota((8, HEAD), 1) == 0)
    ok = jnp.where(jnp.abs(dot_nt(first, x[:, 0:HEAD])) <= QK_MAX, 1.0, 0.0)
    row = jnp.where(ok > 0.0, dot(ok.astype(bf16), upper), -1.0).astype(i32)
    o_ref[...] = dot(ones_where(row[0:1, :] == iota((ROWS, SLOTS), 0)), x).astype(bf16)


def tail_of(x):
    return pl.pallas_call(
        tail_body,
        out_shape=jax.ShapeDtypeStruct((ROWS, 2 * HEAD), bf16),
        grid=(1,),
        in_specs=[pl.BlockSpec((PEERS, PB + UNIT, 2 * HEAD), lambda i: (0, 2, 0))],
        out_specs=pl.BlockSpec((ROWS, 2 * HEAD), lambda i: (0, 0)),
        name="tail",
    )(x)


def compact_body(x_ref, o_ref, tcol_ref):
    lower = ones_where(iota((SLOTS, SLOTS), 1) < iota((SLOTS, SLOTS), 0))
    first = ones_where(iota((8, HEAD), 1) == 0)
    lane = iota((SLOTS, HEAD), 1)
    sub = iota((8, SLOTS), 0)
    row_ok = jnp.zeros((8, SLOTS), f32)
    col_ok = jnp.zeros((SLOTS, HEAD), f32)
    parts = []
    for pair in range(STR // 2):
        both = x_ref[:, pair * 2 * PB : (pair + 1) * 2 * PB, :].astype(f32)
        for half in range(2):
            q = pair * 2 + half
            x = both[:, half * PB : (half + 1) * PB, :].reshape(SLOTS, 2 * HEAD)
            lead = jnp.broadcast_to(x[:, 0:1], (SLOTS, HEAD))
            col_ok = jnp.where((lane == q) & (jnp.abs(lead) <= QK_MAX), 1.0, col_ok)
            x = x.astype(bf16)
            ahead = dot_nt(first, x[:, 0:HEAD])
            row_ok = jnp.where((sub == q) & (jnp.abs(ahead) <= QK_MAX), 1.0, row_ok)
            parts.append(x)
    tcol_ref[...] = jnp.where(col_ok > 0.0, dot(lower, col_ok.astype(bf16)), -1.0)
    trow = jnp.where(row_ok > 0.0, dot_nt(row_ok.astype(bf16), lower), -1.0).astype(i32)
    ids = iota((ROWS, SLOTS), 0)
    for q in range(STR - 1):
        got = dot(ones_where(trow[q : q + 1, :] == ids), parts[q])
        o_ref[q * ROWS : (q + 1) * ROWS, :] = got.astype(bf16)


def compact(x):
    return call(
        compact_body,
        (
            jax.ShapeDtypeStruct(((STR - 1) * ROWS, 2 * HEAD), bf16),
            jax.ShapeDtypeStruct((SLOTS, HEAD), f32),
        ),
        name="compact",
    )(x)


def unit(x):
    x = x.astype(f32)
    return (x * lax.rsqrt(jnp.sum(x * x, axis=1, keepdims=True) + eps_norm)).astype(bf16)


def attend_body(x_ref, tail_ref, halo_ref, tcol_ref, o_ref, out_ref, lse_ref):
    own = iota((ROWS, ROWS), 0) == iota((ROWS, ROWS), 1)
    lane = iota((ROWS, HEAD), 1)
    cols = iota((SLOTS, ROWS), 1)
    lse_ref[:, MSG:, :] = jnp.zeros((PEERS, HEAD - MSG, HEAD), f32)
    prev_k = unit(halo_ref[:, 0:HEAD])
    prev_v = halo_ref[:, HEAD:]
    for q in range(STR):
        here = tail_ref if q == STR - 1 else x_ref.at[q * ROWS : (q + 1) * ROWS]
        qs = here[:, 0:HEAD]
        vs = here[:, HEAD:]
        ks = unit(qs)
        sa = dot_nt(qs, prev_k)
        sb = jnp.where(own, self_score, dot_nt(qs, ks))
        top = jnp.maximum(
            jnp.max(sa, axis=1, keepdims=True), jnp.max(sb, axis=1, keepdims=True)
        )
        pa = jnp.exp(sa - top)
        pb = jnp.exp(sb - top)
        total = jnp.sum(pa, axis=1, keepdims=True) + jnp.sum(pb, axis=1, keepdims=True)
        out = dot(pa.astype(bf16), prev_v) + dot(pb.astype(bf16), vs)
        lse = top + jnp.log(total)
        high = lse.astype(bf16).astype(f32)
        low = lse - high
        side = jnp.where(lane == 0, high, jnp.where(lane == 1, low, 0.0))
        res = jnp.concatenate([(out / total).astype(bf16), side.astype(bf16)], axis=1)
        pick = ones_where(tcol_ref[:, q : q + 1].astype(i32) == cols)
        got = dot(pick, res)
        at = q * PB
        out_ref[:, at : at + PB, :] = got[:, 0:HEAD].reshape(PEERS, PB, HEAD)
        lse_ref[:, at : at + PB, :] = got[:, HEAD:].reshape(PEERS, PB, HEAD)
        prev_k, prev_v = ks, vs
    o_ref[:, 0:MSG, :] = out_ref[...].astype(bf16)
    eye = ones_where(iota((EXTRA, HEAD), 0) == iota((EXTRA, HEAD), 1))

    def side_rows(step, carry):
        for n in range(4):
            p = step * 4 + n
            o_ref[p, MSG:, :] = dot_nt(eye, lse_ref[p].astype(bf16)).astype(bf16)
        return carry

    lax.fori_loop(0, PEERS // 4, side_rows, 0)


def attend(x, tail, halo, tcol):
    return call(
        attend_body,
        jax.ShapeDtypeStruct((PEERS, MSG + EXTRA, HEAD), bf16),
        [pltpu.VMEM((PEERS, MSG, HEAD), f32), pltpu.VMEM((PEERS, HEAD, HEAD), f32)],
        name="attend",
    )(x, tail, halo, tcol)


def unpacked(pos, x_ref, acc_ref, slots):
    acc_ref[...] = x_ref[...].astype(f32)
    packed = x_ref[:, MSG:, :].reshape(PEERS * EXTRA, HEAD)
    peer = pos >> 5
    rest = pos - (peer << 5)
    quarter = rest >> 3
    spot = quarter * PB + iota(pos.shape, 0) * CAP + rest - (quarter << 3)
    cols = jnp.concatenate([pos, peer, spot, spot], axis=0).astype(f32).T.astype(i32)
    lanes = iota((ROWS, PLACES), 1)
    spots = iota((ROWS, HEAD), 1)
    peers = iota((ROWS, PEERS * EXTRA), 1) >> 4
    outs, lses = [], []
    for j in slots:
        pieces = [
            acc_ref[:, q * PB + j * CAP : q * PB + j * CAP + UNIT, :].reshape(PEERS, 1, UNIT, HEAD)
            for q in range(STR)
        ]
        rows = jnp.concatenate(pieces, axis=1).reshape(PLACES, HEAD).astype(bf16)
        outs.append(dot(ones_where(cols[:, j : j + 1] == lanes), rows))
        near = dot_nt(ones_where(cols[:, 8 + j : 9 + j] == spots), packed)
        mine = cols[:, 4 + j : 5 + j] == peers
        lses.append(jnp.sum(jnp.where(mine, near, 0.0), axis=1, keepdims=True))
    return outs, lses


def unpack_body(pos_ref, x_ref, o_ref, lse_ref, acc_ref):
    outs, lses = unpacked(pos_ref[...], x_ref, acc_ref, range(HOPS))
    lane = iota((ROWS, HEAD), 1)
    side = jnp.zeros((ROWS, HEAD), f32)
    for j in range(HOPS):
        o_ref[j] = outs[j].astype(bf16)
        side = jnp.where(lane == j, lses[j], side)
    lse_ref[...] = side


ACC = (PEERS, MSG + EXTRA, HEAD)
HEADS_OUT = (HOPS, ROWS, HEAD)


def unpack(pos, x):
    return call(
        unpack_body,
        (jax.ShapeDtypeStruct(HEADS_OUT, bf16), jax.ShapeDtypeStruct((ROWS, HEAD), f32)),
        [pltpu.VMEM(ACC, f32)],
        name="unpack",
    )(pos, x)


def merge(pos, x, other, other_lse, j):
    def body(pos_ref, x_ref, other_ref, other_lse_ref, o_ref, acc_ref):
        outs, lses = unpacked(pos_ref[...], x_ref, acc_ref, (j,))
        la, lb = other_lse_ref[:, j : j + 1], lses[0]
        top = jnp.maximum(la, lb)
        ea, eb = jnp.exp(la - top), jnp.exp(lb - top)
        o_ref[...] = ((ea * other_ref[0].astype(f32) + eb * outs[0]) / (ea + eb)).astype(bf16)

    whole = lambda *shape: pl.BlockSpec(shape, lambda i: (0,) * len(shape))
    return pl.pallas_call(
        body,
        out_shape=jax.ShapeDtypeStruct((ROWS, HEAD), bf16),
        grid=(1,),
        in_specs=[
            whole(HOPS, ROWS),
            whole(*ACC),
            pl.BlockSpec((1, ROWS, HEAD), lambda i: (j, 0, 0)),
            whole(ROWS, HEAD),
        ],
        out_specs=whole(ROWS, HEAD),
        scratch_shapes=[pltpu.VMEM(ACC, f32)],
        name="merge",
    )(pos, x, other, other_lse)


def join_body(spot_ref, *refs):
    parts, o_ref, sems = refs[:HOPS], refs[HOPS], refs[HOPS + 1]
    copies = []
    for o in range(HOPS):
        head = (spot_ref[1] + o) & (HOPS - 1)
        copies.append(pltpu.make_async_copy(parts[o], o_ref.at[:, lanes_of(head)], sems.at[o]))
    copy_all(copies)


def join_heads(spot, parts):
    return call(
        join_body,
        jax.ShapeDtypeStruct((ROWS, HOPS * HEAD), bf16),
        [pltpu.SemaphoreType.DMA((HOPS,))],
        in_specs=[SMEM] + [HBM] * HOPS,
        out_specs=HBM,
        name="join_heads",
    )(spot, *parts)


NEAR = [[PEERS * j + p for p in range(PEERS)] for j in range(HOPS)]
NEXT = [(PEERS * j + p, PEERS * j + (p + 1) % PEERS) for j in range(HOPS) for p in range(PEERS)]
ORDER = (2, 1, 3)


def hop(x, o):
    count = PEERS * HOPS
    return lax.ppermute(x, "seq", [(s, (s + PEERS * o) % count) for s in range(count)])


def swap(x):
    return lax.all_to_all(x, "seq", 0, 0, tiled=True, axis_index_groups=NEAR)


def on_device(qk, values, dest_dev, dest_slot):
    return routed(qk, values, dest_dev)


def routed(qk, values, dest_dev):
    spot = jnp.stack([lax.axis_index("round"), lax.axis_index("seq") // PEERS]).astype(i32)
    other = lax.ppermute(dest_dev, "round", [(0, 1), (1, 0)])
    mine = list(split_heads(spot, qk, values))
    for o in ORDER:
        mine[o] = hop(mine[o], o)
    here = places(spot, dest_dev, other)
    spots = [here] + [hop(here, o) for o in range(1, HOPS)]
    sent, pos = zip(*[pack(mine, spots, r) for r in range(2)])
    got = [swap(sent[0])]
    tails = [tail_of(got[0])]
    halo = lax.ppermute(tails[0], "seq", NEXT)
    got.append(swap(sent[1]))
    reply = attend(*arranged(got[0], tails[0], halo))
    tails.append(tail_of(got[1]))
    halo = lax.ppermute(tails[1], "seq", NEXT)
    back = [swap(reply)]
    back.append(swap(attend(*arranged(got[1], tails[1], halo))))
    out, lse = unpack(pos[0], back[0])
    done = {}
    for o in ORDER:
        done[o] = hop(merge(pos[1], back[1], out, lse, o), -o)
    done[0] = merge(pos[1], back[1], out, lse, 0)
    return join_heads(spot, [done[o] for o in range(HOPS)])


def arranged(got, tail, halo):
    rows, tcol = compact(got)
    return rows, tail, halo, tcol


def solution(mesh):
    return jax.shard_map(
        on_device,
        mesh=mesh,
        in_specs=(P("seq", None), P("seq", None), P("round", "seq"), P("round", "seq")),
        out_specs=P("seq", "round"),
        check_vma=False,
    )
```

```python
import jax
import jax.numpy as jnp
from jax import lax
from jax.experimental import pallas as pl
from jax.experimental.pallas import tpu as pltpu
from jax.sharding import PartitionSpec as P


HEAD = 128
ROWS = 512
CAP = 6
UNIT = 8
HOPS = 4
PEERS = 32
STR = 4
PB = HOPS * CAP
MSG = STR * PB
SLOTS = PEERS * PB
PLACES = PEERS * STR * UNIT
EXTRA = 16
SIDE = 8
MSG_OUT = MSG + SIDE
QK_MAX = 96.0
PAD_MARK = 1024.0

eps_norm = 1e-06
self_score = -100000.0

bf16 = jnp.bfloat16
f32 = jnp.float32
i32 = jnp.int32


def iota(shape, dim):
    return lax.broadcasted_iota(i32, shape, dim)


def dot(a, b):
    return lax.dot_general(a, b, (((1,), (0,)), ((), ())), preferred_element_type=f32)


def dot_nt(a, b):
    return lax.dot_general(a, b, (((1,), (1,)), ((), ())), preferred_element_type=f32)


def ones_where(mask):
    return jnp.where(mask, 1.0, 0.0).astype(bf16)


def call(body, out_shape, scratch=(), **kw):
    return pl.pallas_call(
        body,
        out_shape=out_shape,
        scratch_shapes=list(scratch),
        compiler_params=pltpu.CompilerParams(vmem_limit_bytes=56 << 20),
        **kw,
    )


def store(ref, value):
    ref[...] = value


def each_peer(body, step=4):
    def some(i, carry):
        for n in range(step):
            body(i * step + n)
        return carry

    lax.fori_loop(0, PEERS // step, some, 0)


def place_rows(dest):
    col = jnp.broadcast_to(dest.astype(f32), (8, ROWS)).T[:, 0:1]
    same = col == dest.astype(f32)
    before = iota((ROWS, ROWS), 0) < iota((ROWS, ROWS), 1)
    rank = jnp.sum(jnp.where(same & before, 1.0, 0.0), axis=0, keepdims=True)
    pos = dest * UNIT + rank.astype(i32)
    high = pos >> 4
    low = pos - high * 16
    half = ROWS // 2
    parts = [x[:, h * half : (h + 1) * half] for h in range(2) for x in (high, low)]
    return jnp.concatenate(parts, axis=0).astype(f32)


def copy_all(copies):
    for c in copies:
        c.start()
    for c in copies:
        c.wait()


def lanes_of(spot):
    return pl.ds(pl.multiple_of(spot * HEAD, HEAD), HEAD)


def split_body(spot_ref, qk_ref, v_ref, *refs):
    outs, sems = refs[:HOPS], refs[HOPS]
    copies = []
    for o in range(HOPS):
        head = spot_ref[0] * HOPS + ((spot_ref[1] + o) & (HOPS - 1))
        for n, ref in enumerate((qk_ref, v_ref)):
            copies.append(
                pltpu.make_async_copy(
                    ref.at[:, lanes_of(head)],
                    outs[o].at[:, n * HEAD : (n + 1) * HEAD],
                    sems.at[o * 2 + n],
                )
            )
    copy_all(copies)


SMEM = pl.BlockSpec(memory_space=pltpu.SMEM)
HBM = pl.BlockSpec(memory_space=pl.ANY)


def split_heads(spot, qk, values):
    return call(
        split_body,
        (jax.ShapeDtypeStruct((ROWS, 2 * HEAD), bf16),) * HOPS,
        [pltpu.SemaphoreType.DMA((2 * HOPS,))],
        in_specs=[SMEM, HBM, HBM],
        name="split_heads",
    )(spot, qk, values)


def place_body(spot_ref, own_ref, other_ref, o_ref):
    own = place_rows(own_ref[...])
    other = place_rows(other_ref[...])
    mine = spot_ref[0] == 0
    o_ref[...] = jnp.concatenate(
        [jnp.where(mine, own, other), jnp.where(mine, other, own), jnp.zeros((8, ROWS // 2), f32)],
        axis=0,
    ).astype(bf16)


def places(spot, own, other):
    vmem = pl.BlockSpec(memory_space=pltpu.VMEM)
    return call(
        place_body,
        jax.ShapeDtypeStruct((EXTRA, 2 * HEAD), bf16),
        in_specs=[SMEM, vmem, vmem],
        name="places",
    )(spot, own, other)


def pack(xs, spots, r):
    def body(*refs):
        x_refs, e_refs = refs[:HOPS], refs[HOPS : 2 * HOPS]
        o_ref, pos_ref, acc_ref = refs[2 * HOPS :]
        ids = iota((PLACES, ROWS), 0)
        ones = jnp.full((ROWS, HEAD), 1.0, bf16)
        for j in range(HOPS):
            rows = e_refs[j][...].astype(f32)[4 * r : 4 * r + 4]
            pos = jnp.concatenate(
                [rows[0:1] * 16.0 + rows[1:2], rows[2:3] * 16.0 + rows[3:4]], axis=1
            ).astype(i32)
            pos_ref[j : j + 1, :] = pos
            pick = ones_where(pos == ids)
            got = dot(pick, x_refs[j][...])
            mark = (1.0 - dot(pick, ones)) * PAD_MARK
            left = (got[:, 0:HEAD] + mark).reshape(PEERS, STR, UNIT, HEAD)
            right = got[:, HEAD:].reshape(PEERS, STR, UNIT, HEAD)
            for q in range(STR):
                at = q * PB + j * CAP
                acc_ref[:, at : at + CAP, 0:HEAD] = left[:, q, 0:CAP, :]
                acc_ref[:, at : at + CAP, HEAD:] = right[:, q, 0:CAP, :]
        each_peer(lambda p: store(o_ref.at[p], acc_ref[p].astype(bf16)))

    shape = (PEERS, MSG, 2 * HEAD)
    return call(
        body,
        (jax.ShapeDtypeStruct(shape, bf16), jax.ShapeDtypeStruct((HOPS, ROWS), i32)),
        [pltpu.VMEM(shape, f32)],
        name="pack",
    )(*xs, *spots)


def tail_body(x_ref, o_ref):
    x = x_ref[...].astype(f32)[:, UNIT:, :].reshape(SLOTS, 2 * HEAD).astype(bf16)
    upper = ones_where(iota((SLOTS, SLOTS), 0) < iota((SLOTS, SLOTS), 1))
    first = ones_where(iota((8, HEAD), 1) == 0)
    ok = jnp.where(jnp.abs(dot_nt(first, x[:, 0:HEAD])) <= QK_MAX, 1.0, 0.0)
    row = jnp.where(ok > 0.0, dot(ok.astype(bf16), upper), -1.0).astype(i32)
    o_ref[...] = dot(ones_where(row[0:1, :] == iota((ROWS, SLOTS), 0)), x).astype(bf16)


def tail_of(x):
    return pl.pallas_call(
        tail_body,
        out_shape=jax.ShapeDtypeStruct((ROWS, 2 * HEAD), bf16),
        grid=(1,),
        in_specs=[pl.BlockSpec((PEERS, PB + UNIT, 2 * HEAD), lambda i: (0, 2, 0))],
        out_specs=pl.BlockSpec((ROWS, 2 * HEAD), lambda i: (0, 0)),
        name="tail",
    )(x)


def compact_body(x_ref, tail_ref, o_ref, tcol_ref):
    lower = ones_where(iota((SLOTS, SLOTS), 1) < iota((SLOTS, SLOTS), 0))
    first = ones_where(iota((8, HEAD), 1) == 0)
    lane = iota((SLOTS, HEAD), 1)
    sub = iota((8, SLOTS), 0)
    row_ok = jnp.zeros((8, SLOTS), f32)
    col_ok = jnp.zeros((SLOTS, HEAD), f32)
    parts = []
    for pair in range(STR // 2):
        both = x_ref[:, pair * 2 * PB : (pair + 1) * 2 * PB, :].astype(f32)
        for half in range(2):
            q = pair * 2 + half
            x = both[:, half * PB : (half + 1) * PB, :].reshape(SLOTS, 2 * HEAD)
            lead = jnp.broadcast_to(x[:, 0:1], (SLOTS, HEAD))
            col_ok = jnp.where((lane == q) & (jnp.abs(lead) <= QK_MAX), 1.0, col_ok)
            x = x.astype(bf16)
            ahead = dot_nt(first, x[:, 0:HEAD])
            row_ok = jnp.where((sub == q) & (jnp.abs(ahead) <= QK_MAX), 1.0, row_ok)
            parts.append(x)
    tcol_ref[...] = jnp.where(col_ok > 0.0, dot(lower, col_ok.astype(bf16)), -1.0)
    trow = jnp.where(row_ok > 0.0, dot_nt(row_ok.astype(bf16), lower), -1.0).astype(i32)
    ids = iota((ROWS, SLOTS), 0)
    for q in range(STR - 1):
        got = dot(ones_where(trow[q : q + 1, :] == ids), parts[q])
        o_ref[q * ROWS : (q + 1) * ROWS, :] = got.astype(bf16)
    o_ref[(STR - 1) * ROWS :, :] = tail_ref[...]


def compact(x, tail):
    return call(
        compact_body,
        (
            jax.ShapeDtypeStruct((STR * ROWS, 2 * HEAD), bf16),
            jax.ShapeDtypeStruct((SLOTS, HEAD), f32),
        ),
        name="compact",
    )(x, tail)


def unit(x):
    x = x.astype(f32)
    return (x * lax.rsqrt(jnp.sum(x * x, axis=1, keepdims=True) + eps_norm)).astype(bf16)


def attend_body(x_ref, halo_ref, tcol_ref, o_ref, out_ref, lse_ref, pk_ref, pv_ref):
    lse_ref[:, MSG:, :] = jnp.zeros((PEERS, HEAD - MSG, HEAD), f32)
    pk_ref[...] = unit(halo_ref[:, 0:HEAD])
    pv_ref[...] = halo_ref[:, HEAD:]

    def one(q, carry):
        here = pl.ds(pl.multiple_of(q * ROWS, ROWS), ROWS)
        qs = x_ref[here, 0:HEAD]
        vs = x_ref[here, HEAD:]
        ks = unit(qs)
        own = iota((ROWS, ROWS), 0) == iota((ROWS, ROWS), 1)
        sa = dot_nt(qs, pk_ref[...])
        sb = jnp.where(own, self_score, dot_nt(qs, ks))
        top = jnp.maximum(
            jnp.max(sa, axis=1, keepdims=True), jnp.max(sb, axis=1, keepdims=True)
        )
        pa = jnp.exp(sa - top)
        pb = jnp.exp(sb - top)
        total = jnp.sum(pa, axis=1, keepdims=True) + jnp.sum(pb, axis=1, keepdims=True)
        out = dot(pa.astype(bf16), pv_ref[...]) + dot(pb.astype(bf16), vs)
        lse = top + jnp.log(total)
        high = lse.astype(bf16).astype(f32)
        low = lse - high
        lane = iota((ROWS, HEAD), 1)
        side = jnp.where(lane == 0, high, jnp.where(lane == 1, low, 0.0))
        res = jnp.concatenate([(out / total).astype(bf16), side.astype(bf16)], axis=1)
        mine = iota((SLOTS, HEAD), 1) == q
        spots = jnp.sum(jnp.where(mine, tcol_ref[...], 0.0), axis=1, keepdims=True)
        got = dot(ones_where(spots.astype(i32) == iota((SLOTS, ROWS), 1)), res)
        at = pl.ds(pl.multiple_of(q * PB, UNIT), PB)
        out_ref[:, at, :] = got[:, 0:HEAD].reshape(PEERS, PB, HEAD)
        lse_ref[:, at, :] = got[:, HEAD:].reshape(PEERS, PB, HEAD)
        pk_ref[...] = ks
        pv_ref[...] = vs
        return carry

    lax.fori_loop(0, STR, one, 0)
    eye = ones_where(iota((SIDE, HEAD), 0) == iota((SIDE, HEAD), 1))

    def send(p):
        o_ref[p, 0:MSG, :] = out_ref[p].astype(bf16)
        o_ref[p, MSG:, :] = dot_nt(eye, lse_ref[p].astype(bf16)).astype(bf16)

    each_peer(send)


def attend(x, halo, tcol):
    return call(
        attend_body,
        jax.ShapeDtypeStruct((PEERS, MSG_OUT, HEAD), bf16),
        [
            pltpu.VMEM((PEERS, MSG, HEAD), f32),
            pltpu.VMEM((PEERS, HEAD, HEAD), f32),
            pltpu.VMEM((ROWS, HEAD), bf16),
            pltpu.VMEM((ROWS, HEAD), bf16),
        ],
        name="attend",
    )(x, halo, tcol)


def unpacked(pos, x_ref, acc_ref, slots):
    each_peer(lambda p: store(acc_ref.at[p], x_ref[p].astype(f32)))
    packed = acc_ref[:, MSG:, :].reshape(PEERS * SIDE, HEAD).astype(bf16)
    peer = pos >> 5
    rest = pos - (peer << 5)
    quarter = rest >> 3
    spot = quarter * PB + iota(pos.shape, 0) * CAP + rest - (quarter << 3)
    cols = jnp.concatenate([pos, peer, spot, spot], axis=0).astype(f32).T.astype(i32)
    lanes = iota((ROWS, PLACES), 1)
    spots = iota((ROWS, HEAD), 1)
    peers = iota((ROWS, PEERS * SIDE), 1) >> 3
    outs, lses = [], []
    for j in slots:
        pieces = [
            acc_ref[:, q * PB + j * CAP : q * PB + j * CAP + UNIT, :].reshape(PEERS, 1, UNIT, HEAD)
            for q in range(STR)
        ]
        rows = jnp.concatenate(pieces, axis=1).reshape(PLACES, HEAD).astype(bf16)
        outs.append(dot(ones_where(cols[:, j : j + 1] == lanes), rows))
        near = dot_nt(ones_where(cols[:, 8 + j : 9 + j] == spots), packed)
        mine = cols[:, 4 + j : 5 + j] == peers
        lses.append(jnp.sum(jnp.where(mine, near, 0.0), axis=1, keepdims=True))
    return outs, lses


def unpack_body(pos_ref, x_ref, o_ref, lse_ref, acc_ref):
    outs, lses = unpacked(pos_ref[...], x_ref, acc_ref, range(HOPS))
    lane = iota((ROWS, HEAD), 1)
    side = jnp.zeros((ROWS, HEAD), f32)
    for j in range(HOPS):
        o_ref[j] = outs[j].astype(bf16)
        side = jnp.where(lane == j, lses[j], side)
    lse_ref[...] = side


ACC = (PEERS, MSG_OUT, HEAD)
HEADS_OUT = (HOPS, ROWS, HEAD)


def unpack(pos, x):
    return call(
        unpack_body,
        (jax.ShapeDtypeStruct(HEADS_OUT, bf16), jax.ShapeDtypeStruct((ROWS, HEAD), f32)),
        [pltpu.VMEM(ACC, f32)],
        name="unpack",
    )(pos, x)


def merge(pos, x, other, other_lse, slots):
    def body(pos_ref, x_ref, other_ref, other_lse_ref, *refs):
        outs, lses = unpacked(pos_ref[...], x_ref, refs[-1], slots)
        for n, j in enumerate(slots):
            la, lb = other_lse_ref[:, j : j + 1], lses[n]
            top = jnp.maximum(la, lb)
            ea, eb = jnp.exp(la - top), jnp.exp(lb - top)
            mix = ea * other_ref[j].astype(f32) + eb * outs[n]
            refs[n][...] = (mix / (ea + eb)).astype(bf16)

    return call(
        body,
        (jax.ShapeDtypeStruct((ROWS, HEAD), bf16),) * len(slots),
        [pltpu.VMEM(ACC, f32)],
        name="merge",
    )(pos, x, other, other_lse)


def join_body(spot_ref, *refs):
    parts, o_ref = refs[:HOPS], refs[HOPS]
    for o in range(HOPS):
        head = (spot_ref[1] + o) & (HOPS - 1)
        o_ref[:, lanes_of(head)] = parts[o][...]


def join_heads(spot, parts):
    vmem = pl.BlockSpec(memory_space=pltpu.VMEM)
    return call(
        join_body,
        jax.ShapeDtypeStruct((ROWS, HOPS * HEAD), bf16),
        in_specs=[SMEM] + [vmem] * HOPS,
        name="join_heads",
    )(spot, *parts)


NEAR = [[PEERS * j + p for p in range(PEERS)] for j in range(HOPS)]
NEXT = [(PEERS * j + p, PEERS * j + (p + 1) % PEERS) for j in range(HOPS) for p in range(PEERS)]
ORDER = (2, 1, 3)


def hop(x, o):
    count = PEERS * HOPS
    return lax.ppermute(x, "seq", [(s, (s + PEERS * o) % count) for s in range(count)])


def swap(x):
    return lax.all_to_all(x, "seq", 0, 0, tiled=True, axis_index_groups=NEAR)


def on_device(qk, values, dest_dev, dest_slot):
    return routed(qk, values, dest_dev)


def routed(qk, values, dest_dev):
    spot = jnp.stack([lax.axis_index("round"), lax.axis_index("seq") // PEERS]).astype(i32)
    other = lax.ppermute(dest_dev, "round", [(0, 1), (1, 0)])
    mine = list(split_heads(spot, qk, values))
    for o in ORDER:
        mine[o] = hop(mine[o], o)
    here = places(spot, dest_dev, other)
    spots = [here] + [hop(here, o) for o in range(1, HOPS)]
    sent, pos = zip(*[pack(mine, spots, r) for r in range(2)])
    got = [swap(sent[0])]
    tails = [tail_of(got[0])]
    halo = lax.ppermute(tails[0], "seq", NEXT)
    got.append(swap(sent[1]))
    reply = attend(*arranged(got[0], tails[0], halo))
    tails.append(tail_of(got[1]))
    halo = lax.ppermute(tails[1], "seq", NEXT)
    back = [swap(reply)]
    back.append(swap(attend(*arranged(got[1], tails[1], halo))))
    out, lse = unpack(pos[0], back[0])
    done = {}
    done[2], done[1] = merge(pos[1], back[1], out, lse, (2, 1))
    for o in (2, 1):
        done[o] = hop(done[o], -o)
    done[3], done[0] = merge(pos[1], back[1], out, lse, (3, 0))
    done[3] = hop(done[3], -3)
    return join_heads(spot, [done[o] for o in range(HOPS)])


def arranged(got, tail, halo):
    rows, tcol = compact(got, tail)
    return rows, halo, tcol


def solution(mesh):
    return jax.shard_map(
        on_device,
        mesh=mesh,
        in_specs=(P("seq", None), P("seq", None), P("round", "seq"), P("round", "seq")),
        out_specs=P("seq", "round"),
        check_vma=False,
    )
```

```python
import jax
import jax.numpy as jnp
from jax import lax
from jax.experimental import pallas as pl
from jax.experimental.pallas import tpu as pltpu
from jax.sharding import PartitionSpec as P


HEAD = 128
ROWS = 512
CAP = 6
UNIT = 8
HOPS = 4
PEERS = 32
STR = 4
PB = HOPS * CAP
MSG = STR * PB
SLOTS = PEERS * PB
PLACES = PEERS * STR * UNIT
GRANT = 16 << 20
EXTRA = 16
SIDE = 8
MSG_OUT = MSG + SIDE
QK_MAX = 96.0
PAD_MARK = 1024.0

eps_norm = 1e-06
self_score = -100000.0

bf16 = jnp.bfloat16
f32 = jnp.float32
i32 = jnp.int32


def iota(shape, dim):
    return lax.broadcasted_iota(i32, shape, dim)


def dot(a, b):
    return lax.dot_general(a, b, (((1,), (0,)), ((), ())), preferred_element_type=f32)


def dot_nt(a, b):
    return lax.dot_general(a, b, (((1,), (1,)), ((), ())), preferred_element_type=f32)


def ones_where(mask):
    return jnp.where(mask, 1.0, 0.0).astype(bf16)


def call(body, out_shape, scratch=(), **kw):
    return pl.pallas_call(
        body,
        out_shape=out_shape,
        scratch_shapes=list(scratch),
        compiler_params=pltpu.CompilerParams(vmem_limit_bytes=GRANT),
        **kw,
    )


def store(ref, value):
    ref[...] = value


def each_peer(body, step=4):
    def some(i, carry):
        for n in range(step):
            body(i * step + n)
        return carry

    lax.fori_loop(0, PEERS // step, some, 0)


def place_rows(dest):
    col = jnp.broadcast_to(dest.astype(f32), (8, ROWS)).T[:, 0:1]
    same = col == dest.astype(f32)
    before = iota((ROWS, ROWS), 0) < iota((ROWS, ROWS), 1)
    rank = jnp.sum(jnp.where(same & before, 1.0, 0.0), axis=0, keepdims=True)
    pos = dest * UNIT + rank.astype(i32)
    high = pos >> 4
    low = pos - high * 16
    half = ROWS // 2
    parts = [x[:, h * half : (h + 1) * half] for h in range(2) for x in (high, low)]
    return jnp.concatenate(parts, axis=0).astype(f32)


def copy_all(copies):
    for c in copies:
        c.start()
    for c in copies:
        c.wait()


def lanes_of(spot):
    return pl.ds(pl.multiple_of(spot * HEAD, HEAD), HEAD)


def split_body(spot_ref, qk_ref, v_ref, *refs):
    outs, sems = refs[:HOPS], refs[HOPS]
    copies = []
    for o in range(HOPS):
        head = spot_ref[0] * HOPS + ((spot_ref[1] + o) & (HOPS - 1))
        for n, ref in enumerate((qk_ref, v_ref)):
            copies.append(
                pltpu.make_async_copy(
                    ref.at[:, lanes_of(head)],
                    outs[o].at[:, n * HEAD : (n + 1) * HEAD],
                    sems.at[o * 2 + n],
                )
            )
    copy_all(copies)


SMEM = pl.BlockSpec(memory_space=pltpu.SMEM)
HBM = pl.BlockSpec(memory_space=pltpu.HBM)


def split_heads(spot, qk, values):
    return call(
        split_body,
        (jax.ShapeDtypeStruct((ROWS, 2 * HEAD), bf16),) * HOPS,
        [pltpu.SemaphoreType.DMA((2 * HOPS,))],
        in_specs=[SMEM, HBM, HBM],
        name="split_heads",
    )(spot, qk, values)


def place_body(spot_ref, own_ref, other_ref, o_ref):
    own = place_rows(own_ref[...])
    other = place_rows(other_ref[...])
    mine = spot_ref[0] == 0
    o_ref[...] = jnp.concatenate(
        [jnp.where(mine, own, other), jnp.where(mine, other, own), jnp.zeros((8, ROWS // 2), f32)],
        axis=0,
    ).astype(bf16)


def places(spot, own, other):
    vmem = pl.BlockSpec(memory_space=pltpu.VMEM)
    return call(
        place_body,
        jax.ShapeDtypeStruct((EXTRA, 2 * HEAD), bf16),
        in_specs=[SMEM, vmem, vmem],
        name="places",
    )(spot, own, other)


def pack(xs, spots, r):
    def body(*refs):
        x_refs, e_refs = refs[:HOPS], refs[HOPS : 2 * HOPS]
        o_ref, pos_ref, acc_ref = refs[2 * HOPS :]
        ids = iota((PLACES, ROWS), 0)
        ones = jnp.full((ROWS, HEAD), 1.0, bf16)
        for j in range(HOPS):
            rows = e_refs[j][...].astype(f32)[4 * r : 4 * r + 4]
            pos = jnp.concatenate(
                [rows[0:1] * 16.0 + rows[1:2], rows[2:3] * 16.0 + rows[3:4]], axis=1
            ).astype(i32)
            pos_ref[j : j + 1, :] = pos
            pick = ones_where(pos == ids)
            got = dot(pick, x_refs[j][...])
            mark = (1.0 - dot(pick, ones)) * PAD_MARK
            left = (got[:, 0:HEAD] + mark).reshape(PEERS, STR, UNIT, HEAD)
            right = got[:, HEAD:].reshape(PEERS, STR, UNIT, HEAD)
            for q in range(STR):
                at = q * PB + j * CAP
                acc_ref[:, at : at + CAP, 0:HEAD] = left[:, q, 0:CAP, :]
                acc_ref[:, at : at + CAP, HEAD:] = right[:, q, 0:CAP, :]
        each_peer(lambda p: store(o_ref.at[p], acc_ref[p].astype(bf16)))

    shape = (PEERS, MSG, 2 * HEAD)
    return call(
        body,
        (jax.ShapeDtypeStruct(shape, bf16), jax.ShapeDtypeStruct((HOPS, ROWS), i32)),
        [pltpu.VMEM(shape, f32)],
        name="pack",
    )(*xs, *spots)


def tail_body(x_ref, o_ref):
    x = x_ref[...].astype(f32)[:, UNIT:, :].reshape(SLOTS, 2 * HEAD).astype(bf16)
    upper = ones_where(iota((SLOTS, SLOTS), 0) < iota((SLOTS, SLOTS), 1))
    first = ones_where(iota((8, HEAD), 1) == 0)
    ok = jnp.where(jnp.abs(dot_nt(first, x[:, 0:HEAD])) <= QK_MAX, 1.0, 0.0)
    row = jnp.where(ok > 0.0, dot(ok.astype(bf16), upper), -1.0).astype(i32)
    o_ref[...] = dot(ones_where(row[0:1, :] == iota((ROWS, SLOTS), 0)), x).astype(bf16)


def tail_of(x):
    return call(
        tail_body,
        jax.ShapeDtypeStruct((ROWS, 2 * HEAD), bf16),
        grid=(1,),
        in_specs=[pl.BlockSpec((PEERS, PB + UNIT, 2 * HEAD), lambda i: (0, 2, 0))],
        out_specs=pl.BlockSpec((ROWS, 2 * HEAD), lambda i: (0, 0)),
        name="tail",
    )(x)


def compact_body(x_ref, tail_ref, o_ref, tcol_ref):
    lower = ones_where(iota((SLOTS, SLOTS), 1) < iota((SLOTS, SLOTS), 0))
    first = ones_where(iota((8, HEAD), 1) == 0)
    lane = iota((SLOTS, HEAD), 1)
    sub = iota((8, SLOTS), 0)
    row_ok = jnp.zeros((8, SLOTS), f32)
    col_ok = jnp.zeros((SLOTS, HEAD), f32)
    parts = []
    for pair in range(STR // 2):
        both = x_ref[:, pair * 2 * PB : (pair + 1) * 2 * PB, :].astype(f32)
        for half in range(2):
            q = pair * 2 + half
            x = both[:, half * PB : (half + 1) * PB, :].reshape(SLOTS, 2 * HEAD)
            lead = jnp.broadcast_to(x[:, 0:1], (SLOTS, HEAD))
            col_ok = jnp.where((lane == q) & (jnp.abs(lead) <= QK_MAX), 1.0, col_ok)
            x = x.astype(bf16)
            ahead = dot_nt(first, x[:, 0:HEAD])
            row_ok = jnp.where((sub == q) & (jnp.abs(ahead) <= QK_MAX), 1.0, row_ok)
            parts.append(x)
    tcol_ref[...] = jnp.where(col_ok > 0.0, dot(lower, col_ok.astype(bf16)), -1.0)
    trow = jnp.where(row_ok > 0.0, dot_nt(row_ok.astype(bf16), lower), -1.0).astype(i32)
    ids = iota((ROWS, SLOTS), 0)
    for q in range(STR - 1):
        got = dot(ones_where(trow[q : q + 1, :] == ids), parts[q])
        o_ref[q * ROWS : (q + 1) * ROWS, :] = got.astype(bf16)
    o_ref[(STR - 1) * ROWS :, :] = tail_ref[...]


def compact(x, tail):
    return call(
        compact_body,
        (
            jax.ShapeDtypeStruct((STR * ROWS, 2 * HEAD), bf16),
            jax.ShapeDtypeStruct((SLOTS, HEAD), f32),
        ),
        name="compact",
    )(x, tail)


def unit(x):
    x = x.astype(f32)
    return (x * lax.rsqrt(jnp.sum(x * x, axis=1, keepdims=True) + eps_norm)).astype(bf16)


def attend_body(x_ref, halo_ref, tcol_ref, o_ref, out_ref, lse_ref, pk_ref, pv_ref):
    lse_ref[:, MSG:, :] = jnp.zeros((PEERS, HEAD - MSG, HEAD), f32)
    pk_ref[...] = unit(halo_ref[:, 0:HEAD])
    pv_ref[...] = halo_ref[:, HEAD:]

    def one(q, carry):
        here = pl.ds(pl.multiple_of(q * ROWS, ROWS), ROWS)
        qs = x_ref[here, 0:HEAD]
        vs = x_ref[here, HEAD:]
        ks = unit(qs)
        own = iota((ROWS, ROWS), 0) == iota((ROWS, ROWS), 1)
        sa = dot_nt(qs, pk_ref[...])
        sb = jnp.where(own, self_score, dot_nt(qs, ks))
        top = jnp.maximum(
            jnp.max(sa, axis=1, keepdims=True), jnp.max(sb, axis=1, keepdims=True)
        )
        pa = jnp.exp(sa - top)
        pb = jnp.exp(sb - top)
        total = jnp.sum(pa, axis=1, keepdims=True) + jnp.sum(pb, axis=1, keepdims=True)
        out = dot(pa.astype(bf16), pv_ref[...]) + dot(pb.astype(bf16), vs)
        lse = top + jnp.log(total)
        high = lse.astype(bf16).astype(f32)
        low = lse - high
        lane = iota((ROWS, HEAD), 1)
        side = jnp.where(lane == 0, high, jnp.where(lane == 1, low, 0.0))
        res = jnp.concatenate([(out / total).astype(bf16), side.astype(bf16)], axis=1)
        mine = iota((SLOTS, HEAD), 1) == q
        spots = jnp.sum(jnp.where(mine, tcol_ref[...], 0.0), axis=1, keepdims=True)
        got = dot(ones_where(spots.astype(i32) == iota((SLOTS, ROWS), 1)), res)
        at = pl.ds(pl.multiple_of(q * PB, UNIT), PB)
        out_ref[:, at, :] = got[:, 0:HEAD].reshape(PEERS, PB, HEAD)
        lse_ref[:, at, :] = got[:, HEAD:].reshape(PEERS, PB, HEAD)
        pk_ref[...] = ks
        pv_ref[...] = vs
        return carry

    lax.fori_loop(0, STR, one, 0)
    eye = ones_where(iota((SIDE, HEAD), 0) == iota((SIDE, HEAD), 1))

    def send(p):
        o_ref[p, 0:MSG, :] = out_ref[p].astype(bf16)
        o_ref[p, MSG:, :] = dot_nt(eye, lse_ref[p].astype(bf16)).astype(bf16)

    each_peer(send)


def attend(x, halo, tcol):
    return call(
        attend_body,
        jax.ShapeDtypeStruct((PEERS, MSG_OUT, HEAD), bf16),
        [
            pltpu.VMEM((PEERS, MSG, HEAD), f32),
            pltpu.VMEM((PEERS, HEAD, HEAD), f32),
            pltpu.VMEM((ROWS, HEAD), bf16),
            pltpu.VMEM((ROWS, HEAD), bf16),
        ],
        name="attend",
    )(x, halo, tcol)


def unpacked(pos, x_ref, acc_ref, slots):
    each_peer(lambda p: store(acc_ref.at[p], x_ref[p].astype(f32)))
    packed = acc_ref[:, MSG:, :].reshape(PEERS * SIDE, HEAD).astype(bf16)
    peer = pos >> 5
    rest = pos - (peer << 5)
    quarter = rest >> 3
    spot = quarter * PB + iota(pos.shape, 0) * CAP + rest - (quarter << 3)
    cols = jnp.concatenate([pos, peer, spot, spot], axis=0).astype(f32).T.astype(i32)
    lanes = iota((ROWS, PLACES), 1)
    spots = iota((ROWS, HEAD), 1)
    peers = iota((ROWS, PEERS * SIDE), 1) >> 3
    outs, lses = [], []
    for j in slots:
        pieces = [
            acc_ref[:, q * PB + j * CAP : q * PB + j * CAP + UNIT, :].reshape(PEERS, 1, UNIT, HEAD)
            for q in range(STR)
        ]
        rows = jnp.concatenate(pieces, axis=1).reshape(PLACES, HEAD).astype(bf16)
        outs.append(dot(ones_where(cols[:, j : j + 1] == lanes), rows))
        near = dot_nt(ones_where(cols[:, 8 + j : 9 + j] == spots), packed)
        mine = cols[:, 4 + j : 5 + j] == peers
        lses.append(jnp.sum(jnp.where(mine, near, 0.0), axis=1, keepdims=True))
    return outs, lses


def unpack_body(pos_ref, x_ref, o_ref, lse_ref, acc_ref):
    outs, lses = unpacked(pos_ref[...], x_ref, acc_ref, range(HOPS))
    lane = iota((ROWS, HEAD), 1)
    side = jnp.zeros((ROWS, HEAD), f32)
    for j in range(HOPS):
        o_ref[j] = outs[j].astype(bf16)
        side = jnp.where(lane == j, lses[j], side)
    lse_ref[...] = side


ACC = (PEERS, MSG_OUT, HEAD)
HEADS_OUT = (HOPS, ROWS, HEAD)


def unpack(pos, x):
    return call(
        unpack_body,
        (jax.ShapeDtypeStruct(HEADS_OUT, bf16), jax.ShapeDtypeStruct((ROWS, HEAD), f32)),
        [pltpu.VMEM(ACC, f32)],
        name="unpack",
    )(pos, x)


def merge(pos, x, other, other_lse, slots):
    def body(pos_ref, x_ref, other_ref, other_lse_ref, *refs):
        outs, lses = unpacked(pos_ref[...], x_ref, refs[-1], slots)
        for n, j in enumerate(slots):
            la, lb = other_lse_ref[:, j : j + 1], lses[n]
            top = jnp.maximum(la, lb)
            ea, eb = jnp.exp(la - top), jnp.exp(lb - top)
            mix = ea * other_ref[j].astype(f32) + eb * outs[n]
            refs[n][...] = (mix / (ea + eb)).astype(bf16)

    return call(
        body,
        (jax.ShapeDtypeStruct((ROWS, HEAD), bf16),) * len(slots),
        [pltpu.VMEM(ACC, f32)],
        name="merge",
    )(pos, x, other, other_lse)


def join_body(spot_ref, *refs):
    parts, o_ref = refs[:HOPS], refs[HOPS]
    for o in range(HOPS):
        head = (spot_ref[1] + o) & (HOPS - 1)
        o_ref[:, lanes_of(head)] = parts[o][...]


def join_heads(spot, parts):
    vmem = pl.BlockSpec(memory_space=pltpu.VMEM)
    return call(
        join_body,
        jax.ShapeDtypeStruct((ROWS, HOPS * HEAD), bf16),
        in_specs=[SMEM] + [vmem] * HOPS,
        name="join_heads",
    )(spot, *parts)


NEAR = [[PEERS * j + p for p in range(PEERS)] for j in range(HOPS)]
NEXT = [(PEERS * j + p, PEERS * j + (p + 1) % PEERS) for j in range(HOPS) for p in range(PEERS)]
ORDER = (2, 1, 3)


def hop(x, o):
    count = PEERS * HOPS
    return lax.ppermute(x, "seq", [(s, (s + PEERS * o) % count) for s in range(count)])


def swap(x):
    return lax.all_to_all(x, "seq", 0, 0, tiled=True, axis_index_groups=NEAR)


def on_device(qk, values, dest_dev, dest_slot):
    return routed(qk, values, dest_dev)


def routed(qk, values, dest_dev):
    spot = jnp.stack([lax.axis_index("round"), lax.axis_index("seq") // PEERS]).astype(i32)
    other = lax.ppermute(dest_dev, "round", [(0, 1), (1, 0)])
    mine = list(split_heads(spot, qk, values))
    for o in ORDER:
        mine[o] = hop(mine[o], o)
    here = places(spot, dest_dev, other)
    spots = [here] + [hop(here, o) for o in range(1, HOPS)]
    sent, pos = zip(*[pack(mine, spots, r) for r in range(2)])
    got = [swap(sent[0])]
    tails = [tail_of(got[0])]
    halo = lax.ppermute(tails[0], "seq", NEXT)
    got.append(swap(sent[1]))
    reply = attend(*arranged(got[0], tails[0], halo))
    tails.append(tail_of(got[1]))
    halo = lax.ppermute(tails[1], "seq", NEXT)
    back = [swap(reply)]
    back.append(swap(attend(*arranged(got[1], tails[1], halo))))
    out, lse = unpack(pos[0], back[0])
    done = {}
    done[2], done[1] = merge(pos[1], back[1], out, lse, (2, 1))
    for o in (2, 1):
        done[o] = hop(done[o], -o)
    done[3], done[0] = merge(pos[1], back[1], out, lse, (3, 0))
    done[3] = hop(done[3], -3)
    return join_heads(spot, [done[o] for o in range(HOPS)])


def arranged(got, tail, halo):
    rows, tcol = compact(got, tail)
    return rows, halo, tcol


def solution(mesh):
    return jax.shard_map(
        on_device,
        mesh=mesh,
        in_specs=(P("seq", None), P("seq", None), P("round", "seq"), P("round", "seq")),
        out_specs=P("seq", "round"),
        check_vma=False,
    )
```

```python
import jax
import jax.numpy as jnp
from jax import lax
from jax.experimental import pallas as pl
from jax.experimental.pallas import tpu as pltpu
from jax.sharding import PartitionSpec as P


HEAD = 128
ROWS = 512
CAP = 6
UNIT = 8
HOPS = 4
PEERS = 32
STR = 4
PB = HOPS * CAP
MSG = STR * PB
SLOTS = PEERS * PB
PLACES = PEERS * STR * UNIT
EXTRA = 16
SIDE = 8
MSG_OUT = MSG + SIDE
QK_MAX = 96.0
PAD_MARK = 1024.0

eps_norm = 1e-06
self_score = -100000.0

bf16 = jnp.bfloat16
f32 = jnp.float32
i32 = jnp.int32


def iota(shape, dim):
    return lax.broadcasted_iota(i32, shape, dim)


def dot(a, b):
    return lax.dot_general(a, b, (((1,), (0,)), ((), ())), preferred_element_type=f32)


def dot_nt(a, b):
    return lax.dot_general(a, b, (((1,), (1,)), ((), ())), preferred_element_type=f32)


def ones_where(mask):
    return jnp.where(mask, 1.0, 0.0).astype(bf16)


def call(body, out_shape, scratch=(), grant=16 << 20, **kw):
    return pl.pallas_call(
        body,
        out_shape=out_shape,
        scratch_shapes=list(scratch),
        compiler_params=pltpu.CompilerParams(vmem_limit_bytes=grant),
        **kw,
    )


def store(ref, value):
    ref[...] = value


def each_peer(body, step=4):
    def some(i, carry):
        for n in range(step):
            body(i * step + n)
        return carry

    lax.fori_loop(0, PEERS // step, some, 0)


def place_rows(dest):
    col = jnp.broadcast_to(dest.astype(f32), (8, ROWS)).T[:, 0:1]
    same = col == dest.astype(f32)
    before = iota((ROWS, ROWS), 0) < iota((ROWS, ROWS), 1)
    rank = jnp.sum(jnp.where(same & before, 1.0, 0.0), axis=0, keepdims=True)
    pos = dest * UNIT + rank.astype(i32)
    high = pos >> 4
    low = pos - high * 16
    half = ROWS // 2
    parts = [x[:, h * half : (h + 1) * half] for h in range(2) for x in (high, low)]
    return jnp.concatenate(parts, axis=0).astype(f32)


def copy_all(copies):
    for c in copies:
        c.start()
    for c in copies:
        c.wait()


def lanes_of(spot):
    return pl.ds(pl.multiple_of(spot * HEAD, HEAD), HEAD)


def split_heads(spot, qk, values, slots):
    def body(spot_ref, qk_ref, v_ref, *refs):
        copies = []
        for i, o in enumerate(slots):
            head = spot_ref[0] * HOPS + ((spot_ref[1] + o) & (HOPS - 1))
            for n, ref in enumerate((qk_ref, v_ref)):
                copies.append(
                    pltpu.make_async_copy(
                        ref.at[:, lanes_of(head)],
                        refs[i].at[:, n * HEAD : (n + 1) * HEAD],
                        refs[-1].at[i * 2 + n],
                    )
                )
        copy_all(copies)

    return call(
        body,
        (jax.ShapeDtypeStruct((ROWS, 2 * HEAD), bf16),) * len(slots),
        [pltpu.SemaphoreType.DMA((2 * len(slots),))],
        grant=56 << 20,
        in_specs=[SMEM, HBM, HBM],
        name="split_heads",
    )(spot, qk, values)


SMEM = pl.BlockSpec(memory_space=pltpu.SMEM)
HBM = pl.BlockSpec(memory_space=pltpu.HBM)


def place_body(spot_ref, own_ref, other_ref, o_ref):
    own = place_rows(own_ref[...])
    other = place_rows(other_ref[...])
    mine = spot_ref[0] == 0
    o_ref[...] = jnp.concatenate(
        [jnp.where(mine, own, other), jnp.where(mine, other, own), jnp.zeros((8, ROWS // 2), f32)],
        axis=0,
    ).astype(bf16)


def places(spot, own, other):
    vmem = pl.BlockSpec(memory_space=pltpu.VMEM)
    return call(
        place_body,
        jax.ShapeDtypeStruct((EXTRA, 2 * HEAD), bf16),
        in_specs=[SMEM, vmem, vmem],
        name="places",
    )(spot, own, other)


def pack(xs, spots, r):
    def body(*refs):
        x_refs, e_refs = refs[:HOPS], refs[HOPS : 2 * HOPS]
        o_ref, pos_ref, acc_ref = refs[2 * HOPS :]
        ids = iota((PLACES, ROWS), 0)
        ones = jnp.full((ROWS, HEAD), 1.0, bf16)
        for j in range(HOPS):
            rows = e_refs[j][...].astype(f32)[4 * r : 4 * r + 4]
            pos = jnp.concatenate(
                [rows[0:1] * 16.0 + rows[1:2], rows[2:3] * 16.0 + rows[3:4]], axis=1
            ).astype(i32)
            pos_ref[j : j + 1, :] = pos
            pick = ones_where(pos == ids)
            got = dot(pick, x_refs[j][...])
            mark = (1.0 - dot(pick, ones)) * PAD_MARK
            left = (got[:, 0:HEAD] + mark).reshape(PEERS, STR, UNIT, HEAD)
            right = got[:, HEAD:].reshape(PEERS, STR, UNIT, HEAD)
            for q in range(STR):
                at = q * PB + j * CAP
                acc_ref[:, at : at + CAP, 0:HEAD] = left[:, q, 0:CAP, :]
                acc_ref[:, at : at + CAP, HEAD:] = right[:, q, 0:CAP, :]
        each_peer(lambda p: store(o_ref.at[p], acc_ref[p].astype(bf16)))

    shape = (PEERS, MSG, 2 * HEAD)
    return call(
        body,
        (jax.ShapeDtypeStruct(shape, bf16), jax.ShapeDtypeStruct((HOPS, ROWS), i32)),
        [pltpu.VMEM(shape, f32)],
        name="pack",
    )(*xs, *spots)


def tail_body(x_ref, o_ref):
    x = x_ref[...].astype(f32)[:, UNIT:, :].reshape(SLOTS, 2 * HEAD).astype(bf16)
    upper = ones_where(iota((SLOTS, SLOTS), 0) < iota((SLOTS, SLOTS), 1))
    first = ones_where(iota((8, HEAD), 1) == 0)
    ok = jnp.where(jnp.abs(dot_nt(first, x[:, 0:HEAD])) <= QK_MAX, 1.0, 0.0)
    row = jnp.where(ok > 0.0, dot(ok.astype(bf16), upper), -1.0).astype(i32)
    o_ref[...] = dot(ones_where(row[0:1, :] == iota((ROWS, SLOTS), 0)), x).astype(bf16)


def tail_of(x):
    return call(
        tail_body,
        jax.ShapeDtypeStruct((ROWS, 2 * HEAD), bf16),
        grid=(1,),
        in_specs=[pl.BlockSpec((PEERS, PB + UNIT, 2 * HEAD), lambda i: (0, 2, 0))],
        out_specs=pl.BlockSpec((ROWS, 2 * HEAD), lambda i: (0, 0)),
        name="tail",
    )(x)


def compact_body(x_ref, tail_ref, o_ref, tcol_ref):
    lower = ones_where(iota((SLOTS, SLOTS), 1) < iota((SLOTS, SLOTS), 0))
    first = ones_where(iota((8, HEAD), 1) == 0)
    lane = iota((SLOTS, HEAD), 1)
    sub = iota((8, SLOTS), 0)
    row_ok = jnp.zeros((8, SLOTS), f32)
    col_ok = jnp.zeros((SLOTS, HEAD), f32)
    parts = []
    for pair in range(STR // 2):
        both = x_ref[:, pair * 2 * PB : (pair + 1) * 2 * PB, :].astype(f32)
        for half in range(2):
            q = pair * 2 + half
            x = both[:, half * PB : (half + 1) * PB, :].reshape(SLOTS, 2 * HEAD)
            lead = jnp.broadcast_to(x[:, 0:1], (SLOTS, HEAD))
            col_ok = jnp.where((lane == q) & (jnp.abs(lead) <= QK_MAX), 1.0, col_ok)
            x = x.astype(bf16)
            ahead = dot_nt(first, x[:, 0:HEAD])
            row_ok = jnp.where((sub == q) & (jnp.abs(ahead) <= QK_MAX), 1.0, row_ok)
            parts.append(x)
    tcol_ref[...] = jnp.where(col_ok > 0.0, dot(lower, col_ok.astype(bf16)), -1.0)
    trow = jnp.where(row_ok > 0.0, dot_nt(row_ok.astype(bf16), lower), -1.0).astype(i32)
    ids = iota((ROWS, SLOTS), 0)
    for q in range(STR - 1):
        got = dot(ones_where(trow[q : q + 1, :] == ids), parts[q])
        o_ref[q * ROWS : (q + 1) * ROWS, :] = got.astype(bf16)
    o_ref[(STR - 1) * ROWS :, :] = tail_ref[...]


def compact(x, tail):
    return call(
        compact_body,
        (
            jax.ShapeDtypeStruct((STR * ROWS, 2 * HEAD), bf16),
            jax.ShapeDtypeStruct((SLOTS, HEAD), f32),
        ),
        name="compact",
    )(x, tail)


def unit(x):
    x = x.astype(f32)
    return (x * lax.rsqrt(jnp.sum(x * x, axis=1, keepdims=True) + eps_norm)).astype(bf16)


def attend_body(x_ref, halo_ref, tcol_ref, o_ref, out_ref, lse_ref, pk_ref, pv_ref):
    lse_ref[:, MSG:, :] = jnp.zeros((PEERS, HEAD - MSG, HEAD), f32)
    pk_ref[...] = unit(halo_ref[:, 0:HEAD])
    pv_ref[...] = halo_ref[:, HEAD:]

    def one(q, carry):
        here = pl.ds(pl.multiple_of(q * ROWS, ROWS), ROWS)
        qs = x_ref[here, 0:HEAD]
        vs = x_ref[here, HEAD:]
        ks = unit(qs)
        own = iota((ROWS, ROWS), 0) == iota((ROWS, ROWS), 1)
        sa = dot_nt(qs, pk_ref[...])
        sb = jnp.where(own, self_score, dot_nt(qs, ks))
        top = jnp.maximum(
            jnp.max(sa, axis=1, keepdims=True), jnp.max(sb, axis=1, keepdims=True)
        )
        pa = jnp.exp(sa - top)
        pb = jnp.exp(sb - top)
        total = jnp.sum(pa, axis=1, keepdims=True) + jnp.sum(pb, axis=1, keepdims=True)
        out = dot(pa.astype(bf16), pv_ref[...]) + dot(pb.astype(bf16), vs)
        lse = top + jnp.log(total)
        high = lse.astype(bf16).astype(f32)
        low = lse - high
        lane = iota((ROWS, HEAD), 1)
        side = jnp.where(lane == 0, high, jnp.where(lane == 1, low, 0.0))
        res = jnp.concatenate([(out / total).astype(bf16), side.astype(bf16)], axis=1)
        mine = iota((SLOTS, HEAD), 1) == q
        spots = jnp.sum(jnp.where(mine, tcol_ref[...], 0.0), axis=1, keepdims=True)
        got = dot(ones_where(spots.astype(i32) == iota((SLOTS, ROWS), 1)), res)
        at = pl.ds(pl.multiple_of(q * PB, UNIT), PB)
        out_ref[:, at, :] = got[:, 0:HEAD].reshape(PEERS, PB, HEAD)
        lse_ref[:, at, :] = got[:, HEAD:].reshape(PEERS, PB, HEAD)
        pk_ref[...] = ks
        pv_ref[...] = vs
        return carry

    lax.fori_loop(0, STR, one, 0)
    eye = ones_where(iota((SIDE, HEAD), 0) == iota((SIDE, HEAD), 1))

    def send(p):
        o_ref[p, 0:MSG, :] = out_ref[p].astype(bf16)
        o_ref[p, MSG:, :] = dot_nt(eye, lse_ref[p].astype(bf16)).astype(bf16)

    each_peer(send)


def attend(x, halo, tcol):
    return call(
        attend_body,
        jax.ShapeDtypeStruct((PEERS, MSG_OUT, HEAD), bf16),
        [
            pltpu.VMEM((PEERS, MSG, HEAD), f32),
            pltpu.VMEM((PEERS, HEAD, HEAD), f32),
            pltpu.VMEM((ROWS, HEAD), bf16),
            pltpu.VMEM((ROWS, HEAD), bf16),
        ],
        name="attend",
    )(x, halo, tcol)


def unpacked(pos, x_ref, acc_ref, slots):
    each_peer(lambda p: store(acc_ref.at[p], x_ref[p].astype(f32)))
    packed = acc_ref[:, MSG:, :].reshape(PEERS * SIDE, HEAD).astype(bf16)
    peer = pos >> 5
    rest = pos - (peer << 5)
    quarter = rest >> 3
    spot = quarter * PB + iota(pos.shape, 0) * CAP + rest - (quarter << 3)
    cols = jnp.concatenate([pos, peer, spot, spot], axis=0).astype(f32).T.astype(i32)
    lanes = iota((ROWS, PLACES), 1)
    spots = iota((ROWS, HEAD), 1)
    peers = iota((ROWS, PEERS * SIDE), 1) >> 3
    outs, lses = [], []
    for j in slots:
        pieces = [
            acc_ref[:, q * PB + j * CAP : q * PB + j * CAP + UNIT, :].reshape(PEERS, 1, UNIT, HEAD)
            for q in range(STR)
        ]
        rows = jnp.concatenate(pieces, axis=1).reshape(PLACES, HEAD).astype(bf16)
        outs.append(dot(ones_where(cols[:, j : j + 1] == lanes), rows))
        near = dot_nt(ones_where(cols[:, 8 + j : 9 + j] == spots), packed)
        mine = cols[:, 4 + j : 5 + j] == peers
        lses.append(jnp.sum(jnp.where(mine, near, 0.0), axis=1, keepdims=True))
    return outs, lses


def unpack_body(pos_ref, x_ref, o_ref, lse_ref, acc_ref):
    outs, lses = unpacked(pos_ref[...], x_ref, acc_ref, range(HOPS))
    lane = iota((ROWS, HEAD), 1)
    side = jnp.zeros((ROWS, HEAD), f32)
    for j in range(HOPS):
        o_ref[j] = outs[j].astype(bf16)
        side = jnp.where(lane == j, lses[j], side)
    lse_ref[...] = side


ACC = (PEERS, MSG_OUT, HEAD)
HEADS_OUT = (HOPS, ROWS, HEAD)


def unpack(pos, x):
    return call(
        unpack_body,
        (jax.ShapeDtypeStruct(HEADS_OUT, bf16), jax.ShapeDtypeStruct((ROWS, HEAD), f32)),
        [pltpu.VMEM(ACC, f32)],
        name="unpack",
    )(pos, x)


def merge(pos, x, other, other_lse, slots):
    def body(pos_ref, x_ref, other_ref, other_lse_ref, *refs):
        outs, lses = unpacked(pos_ref[...], x_ref, refs[-1], slots)
        for n, j in enumerate(slots):
            la, lb = other_lse_ref[:, j : j + 1], lses[n]
            top = jnp.maximum(la, lb)
            ea, eb = jnp.exp(la - top), jnp.exp(lb - top)
            mix = ea * other_ref[j].astype(f32) + eb * outs[n]
            refs[n][...] = (mix / (ea + eb)).astype(bf16)

    return call(
        body,
        (jax.ShapeDtypeStruct((ROWS, HEAD), bf16),) * len(slots),
        [pltpu.VMEM(ACC, f32)],
        name="merge",
    )(pos, x, other, other_lse)


def join_body(spot_ref, *refs):
    parts, o_ref = refs[:HOPS], refs[HOPS]
    for o in range(HOPS):
        head = (spot_ref[1] + o) & (HOPS - 1)
        o_ref[:, lanes_of(head)] = parts[o][...]


def join_heads(spot, parts):
    vmem = pl.BlockSpec(memory_space=pltpu.VMEM)
    return call(
        join_body,
        jax.ShapeDtypeStruct((ROWS, HOPS * HEAD), bf16),
        in_specs=[SMEM] + [vmem] * HOPS,
        name="join_heads",
    )(spot, *parts)


NEAR = [[PEERS * j + p for p in range(PEERS)] for j in range(HOPS)]
NEXT = [(PEERS * j + p, PEERS * j + (p + 1) % PEERS) for j in range(HOPS) for p in range(PEERS)]


def hop(x, o):
    count = PEERS * HOPS
    return lax.ppermute(x, "seq", [(s, (s + PEERS * o) % count) for s in range(count)])


def swap(x):
    return lax.all_to_all(x, "seq", 0, 0, tiled=True, axis_index_groups=NEAR)


def on_device(qk, values, dest_dev, dest_slot):
    return routed(qk, values, dest_dev)


def routed(qk, values, dest_dev):
    spot = jnp.stack([lax.axis_index("round"), lax.axis_index("seq") // PEERS]).astype(i32)
    other = lax.ppermute(dest_dev, "round", [(0, 1), (1, 0)])
    mine = {}
    (mine[2],) = split_heads(spot, qk, values, (2,))
    mine[2] = hop(mine[2], 2)
    mine[1], mine[3], mine[0] = split_heads(spot, qk, values, (1, 3, 0))
    for o in (1, 3):
        mine[o] = hop(mine[o], o)
    mine = [mine[o] for o in range(HOPS)]
    here = places(spot, dest_dev, other)
    spots = [here] + [hop(here, o) for o in range(1, HOPS)]
    sent, pos = zip(*[pack(mine, spots, r) for r in range(2)])
    got = [swap(sent[0])]
    tails = [tail_of(got[0])]
    halo = lax.ppermute(tails[0], "seq", NEXT)
    got.append(swap(sent[1]))
    reply = attend(*arranged(got[0], tails[0], halo))
    tails.append(tail_of(got[1]))
    halo = lax.ppermute(tails[1], "seq", NEXT)
    back = [swap(reply)]
    back.append(swap(attend(*arranged(got[1], tails[1], halo))))
    out, lse = unpack(pos[0], back[0])
    done = {}
    done[2], done[1] = merge(pos[1], back[1], out, lse, (2, 1))
    for o in (2, 1):
        done[o] = hop(done[o], -o)
    done[3], done[0] = merge(pos[1], back[1], out, lse, (3, 0))
    done[3] = hop(done[3], -3)
    return join_heads(spot, [done[o] for o in range(HOPS)])


def arranged(got, tail, halo):
    rows, tcol = compact(got, tail)
    return rows, halo, tcol


def solution(mesh):
    return jax.shard_map(
        on_device,
        mesh=mesh,
        in_specs=(P("seq", None), P("seq", None), P("round", "seq"), P("round", "seq")),
        out_specs=P("seq", "round"),
        check_vma=False,
    )
```

```python
import jax
import jax.numpy as jnp
from jax import lax
from jax.experimental import pallas as pl
from jax.experimental.pallas import tpu as pltpu
from jax.sharding import PartitionSpec as P


HEAD = 128
ROWS = 512
CAP = 6
UNIT = 8
HOPS = 4
PEERS = 32
STR = 4
PB = HOPS * CAP
MSG = STR * PB
SLOTS = PEERS * PB
PLACES = PEERS * STR * UNIT
EXTRA = 16
SIDE = 8
MSG_OUT = MSG + SIDE
QK_MAX = 96.0
PAD_MARK = 1024.0

eps_norm = 1e-06
self_score = -100000.0

bf16 = jnp.bfloat16
f32 = jnp.float32
i32 = jnp.int32


def iota(shape, dim):
    return lax.broadcasted_iota(i32, shape, dim)


def dot(a, b):
    return lax.dot_general(a, b, (((1,), (0,)), ((), ())), preferred_element_type=f32)


def dot_nt(a, b):
    return lax.dot_general(a, b, (((1,), (1,)), ((), ())), preferred_element_type=f32)


def ones_where(mask):
    return jnp.where(mask, 1.0, 0.0).astype(bf16)


def call(body, out_shape, scratch=(), grant=16 << 20, **kw):
    return pl.pallas_call(
        body,
        out_shape=out_shape,
        scratch_shapes=list(scratch),
        compiler_params=pltpu.CompilerParams(vmem_limit_bytes=grant),
        **kw,
    )


def store(ref, value):
    ref[...] = value


def each_peer(body, step=4):
    def some(i, carry):
        for n in range(step):
            body(i * step + n)
        return carry

    lax.fori_loop(0, PEERS // step, some, 0)


def place_rows(dest):
    col = jnp.broadcast_to(dest.astype(f32), (8, ROWS)).T[:, 0:1]
    same = col == dest.astype(f32)
    before = iota((ROWS, ROWS), 0) < iota((ROWS, ROWS), 1)
    rank = jnp.sum(jnp.where(same & before, 1.0, 0.0), axis=0, keepdims=True)
    pos = dest * UNIT + rank.astype(i32)
    high = pos >> 4
    low = pos - high * 16
    half = ROWS // 2
    parts = [x[:, h * half : (h + 1) * half] for h in range(2) for x in (high, low)]
    return jnp.concatenate(parts, axis=0).astype(f32)


def copy_all(copies):
    for c in copies:
        c.start()
    for c in copies:
        c.wait()


def lanes_of(spot):
    return pl.ds(pl.multiple_of(spot * HEAD, HEAD), HEAD)


def split_heads(spot, qk, values, slots, grant=56 << 20):
    def body(spot_ref, qk_ref, v_ref, *refs):
        copies = []
        for i, o in enumerate(slots):
            head = spot_ref[0] * HOPS + ((spot_ref[1] + o) & (HOPS - 1))
            for n, ref in enumerate((qk_ref, v_ref)):
                copies.append(
                    pltpu.make_async_copy(
                        ref.at[:, lanes_of(head)],
                        refs[i].at[:, n * HEAD : (n + 1) * HEAD],
                        refs[-1].at[i * 2 + n],
                    )
                )
        copy_all(copies)

    return call(
        body,
        (jax.ShapeDtypeStruct((ROWS, 2 * HEAD), bf16),) * len(slots),
        [pltpu.SemaphoreType.DMA((2 * len(slots),))],
        grant=grant,
        in_specs=[SMEM, HBM, HBM],
        name="split_heads",
    )(spot, qk, values)


SMEM = pl.BlockSpec(memory_space=pltpu.SMEM)
HBM = pl.BlockSpec(memory_space=pltpu.HBM)


def place_body(spot_ref, own_ref, other_ref, o_ref):
    own = place_rows(own_ref[...])
    other = place_rows(other_ref[...])
    mine = spot_ref[0] == 0
    o_ref[...] = jnp.concatenate(
        [jnp.where(mine, own, other), jnp.where(mine, other, own), jnp.zeros((8, ROWS // 2), f32)],
        axis=0,
    ).astype(bf16)


def places(spot, own, other):
    vmem = pl.BlockSpec(memory_space=pltpu.VMEM)
    return call(
        place_body,
        jax.ShapeDtypeStruct((EXTRA, 2 * HEAD), bf16),
        in_specs=[SMEM, vmem, vmem],
        name="places",
    )(spot, own, other)


def pack(xs, spots, r):
    def body(*refs):
        x_refs, e_refs = refs[:HOPS], refs[HOPS : 2 * HOPS]
        o_ref, pos_ref, acc_ref = refs[2 * HOPS :]
        ids = iota((PLACES, ROWS), 0)
        ones = jnp.full((ROWS, HEAD), 1.0, bf16)
        for j in range(HOPS):
            rows = e_refs[j][...].astype(f32)[4 * r : 4 * r + 4]
            pos = jnp.concatenate(
                [rows[0:1] * 16.0 + rows[1:2], rows[2:3] * 16.0 + rows[3:4]], axis=1
            ).astype(i32)
            pos_ref[j : j + 1, :] = pos
            pick = ones_where(pos == ids)
            got = dot(pick, x_refs[j][...])
            mark = (1.0 - dot(pick, ones)) * PAD_MARK
            left = (got[:, 0:HEAD] + mark).reshape(PEERS, STR, UNIT, HEAD)
            right = got[:, HEAD:].reshape(PEERS, STR, UNIT, HEAD)
            for q in range(STR):
                at = q * PB + j * CAP
                acc_ref[:, at : at + CAP, 0:HEAD] = left[:, q, 0:CAP, :]
                acc_ref[:, at : at + CAP, HEAD:] = right[:, q, 0:CAP, :]
        each_peer(lambda p: store(o_ref.at[p], acc_ref[p].astype(bf16)))

    shape = (PEERS, MSG, 2 * HEAD)
    return call(
        body,
        (jax.ShapeDtypeStruct(shape, bf16), jax.ShapeDtypeStruct((HOPS, ROWS), i32)),
        [pltpu.VMEM(shape, f32)],
        name="pack",
    )(*xs, *spots)


def tail_body(x_ref, o_ref):
    x = x_ref[...].astype(f32)[:, UNIT:, :].reshape(SLOTS, 2 * HEAD).astype(bf16)
    upper = ones_where(iota((SLOTS, SLOTS), 0) < iota((SLOTS, SLOTS), 1))
    first = ones_where(iota((8, HEAD), 1) == 0)
    ok = jnp.where(jnp.abs(dot_nt(first, x[:, 0:HEAD])) <= QK_MAX, 1.0, 0.0)
    row = jnp.where(ok > 0.0, dot(ok.astype(bf16), upper), -1.0).astype(i32)
    o_ref[...] = dot(ones_where(row[0:1, :] == iota((ROWS, SLOTS), 0)), x).astype(bf16)


def tail_of(x):
    return call(
        tail_body,
        jax.ShapeDtypeStruct((ROWS, 2 * HEAD), bf16),
        grid=(1,),
        in_specs=[pl.BlockSpec((PEERS, PB + UNIT, 2 * HEAD), lambda i: (0, 2, 0))],
        out_specs=pl.BlockSpec((ROWS, 2 * HEAD), lambda i: (0, 0)),
        name="tail",
    )(x)


def compact_body(x_ref, tail_ref, o_ref, tcol_ref):
    lower = ones_where(iota((SLOTS, SLOTS), 1) < iota((SLOTS, SLOTS), 0))
    first = ones_where(iota((8, HEAD), 1) == 0)
    lane = iota((SLOTS, HEAD), 1)
    sub = iota((8, SLOTS), 0)
    row_ok = jnp.zeros((8, SLOTS), f32)
    col_ok = jnp.zeros((SLOTS, HEAD), f32)
    parts = []
    for pair in range(STR // 2):
        both = x_ref[:, pair * 2 * PB : (pair + 1) * 2 * PB, :].astype(f32)
        for half in range(2):
            q = pair * 2 + half
            x = both[:, half * PB : (half + 1) * PB, :].reshape(SLOTS, 2 * HEAD)
            lead = jnp.broadcast_to(x[:, 0:1], (SLOTS, HEAD))
            col_ok = jnp.where((lane == q) & (jnp.abs(lead) <= QK_MAX), 1.0, col_ok)
            x = x.astype(bf16)
            ahead = dot_nt(first, x[:, 0:HEAD])
            row_ok = jnp.where((sub == q) & (jnp.abs(ahead) <= QK_MAX), 1.0, row_ok)
            parts.append(x)
    tcol_ref[...] = jnp.where(col_ok > 0.0, dot(lower, col_ok.astype(bf16)), -1.0)
    trow = jnp.where(row_ok > 0.0, dot_nt(row_ok.astype(bf16), lower), -1.0).astype(i32)
    ids = iota((ROWS, SLOTS), 0)
    for q in range(STR - 1):
        got = dot(ones_where(trow[q : q + 1, :] == ids), parts[q])
        o_ref[q * ROWS : (q + 1) * ROWS, :] = got.astype(bf16)
    o_ref[(STR - 1) * ROWS :, :] = tail_ref[...]


def compact(x, tail):
    return call(
        compact_body,
        (
            jax.ShapeDtypeStruct((STR * ROWS, 2 * HEAD), bf16),
            jax.ShapeDtypeStruct((SLOTS, HEAD), f32),
        ),
        name="compact",
    )(x, tail)


def unit(x):
    x = x.astype(f32)
    return (x * lax.rsqrt(jnp.sum(x * x, axis=1, keepdims=True) + eps_norm)).astype(bf16)


def attend_body(x_ref, halo_ref, tcol_ref, o_ref, out_ref, lse_ref, pk_ref, pv_ref):
    lse_ref[:, MSG:, :] = jnp.zeros((PEERS, HEAD - MSG, HEAD), f32)
    pk_ref[...] = unit(halo_ref[:, 0:HEAD])
    pv_ref[...] = halo_ref[:, HEAD:]

    def one(q, carry):
        here = pl.ds(pl.multiple_of(q * ROWS, ROWS), ROWS)
        qs = x_ref[here, 0:HEAD]
        vs = x_ref[here, HEAD:]
        ks = unit(qs)
        own = iota((ROWS, ROWS), 0) == iota((ROWS, ROWS), 1)
        sa = dot_nt(qs, pk_ref[...])
        sb = jnp.where(own, self_score, dot_nt(qs, ks))
        top = jnp.maximum(
            jnp.max(sa, axis=1, keepdims=True), jnp.max(sb, axis=1, keepdims=True)
        )
        pa = jnp.exp(sa - top)
        pb = jnp.exp(sb - top)
        total = jnp.sum(pa, axis=1, keepdims=True) + jnp.sum(pb, axis=1, keepdims=True)
        out = dot(pa.astype(bf16), pv_ref[...]) + dot(pb.astype(bf16), vs)
        lse = top + jnp.log(total)
        high = lse.astype(bf16).astype(f32)
        low = lse - high
        lane = iota((ROWS, HEAD), 1)
        side = jnp.where(lane == 0, high, jnp.where(lane == 1, low, 0.0))
        res = jnp.concatenate([(out / total).astype(bf16), side.astype(bf16)], axis=1)
        mine = iota((SLOTS, HEAD), 1) == q
        spots = jnp.sum(jnp.where(mine, tcol_ref[...], 0.0), axis=1, keepdims=True)
        got = dot(ones_where(spots.astype(i32) == iota((SLOTS, ROWS), 1)), res)
        at = pl.ds(pl.multiple_of(q * PB, UNIT), PB)
        out_ref[:, at, :] = got[:, 0:HEAD].reshape(PEERS, PB, HEAD)
        lse_ref[:, at, :] = got[:, HEAD:].reshape(PEERS, PB, HEAD)
        pk_ref[...] = ks
        pv_ref[...] = vs
        return carry

    lax.fori_loop(0, STR, one, 0)
    eye = ones_where(iota((SIDE, HEAD), 0) == iota((SIDE, HEAD), 1))

    def send(p):
        o_ref[p, 0:MSG, :] = out_ref[p].astype(bf16)
        o_ref[p, MSG:, :] = dot_nt(eye, lse_ref[p].astype(bf16)).astype(bf16)

    each_peer(send)


def attend(x, halo, tcol):
    return call(
        attend_body,
        jax.ShapeDtypeStruct((PEERS, MSG_OUT, HEAD), bf16),
        [
            pltpu.VMEM((PEERS, MSG, HEAD), f32),
            pltpu.VMEM((PEERS, HEAD, HEAD), f32),
            pltpu.VMEM((ROWS, HEAD), bf16),
            pltpu.VMEM((ROWS, HEAD), bf16),
        ],
        name="attend",
    )(x, halo, tcol)


def unpacked(pos, x_ref, acc_ref, slots):
    each_peer(lambda p: store(acc_ref.at[p], x_ref[p].astype(f32)))
    packed = acc_ref[:, MSG:, :].reshape(PEERS * SIDE, HEAD).astype(bf16)
    peer = pos >> 5
    rest = pos - (peer << 5)
    quarter = rest >> 3
    spot = quarter * PB + iota(pos.shape, 0) * CAP + rest - (quarter << 3)
    cols = jnp.concatenate([pos, peer, spot, spot], axis=0).astype(f32).T.astype(i32)
    lanes = iota((ROWS, PLACES), 1)
    spots = iota((ROWS, HEAD), 1)
    peers = iota((ROWS, PEERS * SIDE), 1) >> 3
    outs, lses = [], []
    for j in slots:
        pieces = [
            acc_ref[:, q * PB + j * CAP : q * PB + j * CAP + UNIT, :].reshape(PEERS, 1, UNIT, HEAD)
            for q in range(STR)
        ]
        rows = jnp.concatenate(pieces, axis=1).reshape(PLACES, HEAD).astype(bf16)
        outs.append(dot(ones_where(cols[:, j : j + 1] == lanes), rows))
        near = dot_nt(ones_where(cols[:, 8 + j : 9 + j] == spots), packed)
        mine = cols[:, 4 + j : 5 + j] == peers
        lses.append(jnp.sum(jnp.where(mine, near, 0.0), axis=1, keepdims=True))
    return outs, lses


def unpack_body(pos_ref, x_ref, o_ref, lse_ref, acc_ref):
    outs, lses = unpacked(pos_ref[...], x_ref, acc_ref, range(HOPS))
    lane = iota((ROWS, HEAD), 1)
    side = jnp.zeros((ROWS, HEAD), f32)
    for j in range(HOPS):
        o_ref[j] = outs[j].astype(bf16)
        side = jnp.where(lane == j, lses[j], side)
    lse_ref[...] = side


ACC = (PEERS, MSG_OUT, HEAD)
HEADS_OUT = (HOPS, ROWS, HEAD)


def unpack(pos, x):
    return call(
        unpack_body,
        (jax.ShapeDtypeStruct(HEADS_OUT, bf16), jax.ShapeDtypeStruct((ROWS, HEAD), f32)),
        [pltpu.VMEM(ACC, f32)],
        name="unpack",
    )(pos, x)


def merge(pos, x, other, other_lse, slots):
    def body(pos_ref, x_ref, other_ref, other_lse_ref, *refs):
        outs, lses = unpacked(pos_ref[...], x_ref, refs[-1], slots)
        for n, j in enumerate(slots):
            la, lb = other_lse_ref[:, j : j + 1], lses[n]
            top = jnp.maximum(la, lb)
            ea, eb = jnp.exp(la - top), jnp.exp(lb - top)
            mix = ea * other_ref[j].astype(f32) + eb * outs[n]
            refs[n][...] = (mix / (ea + eb)).astype(bf16)

    return call(
        body,
        (jax.ShapeDtypeStruct((ROWS, HEAD), bf16),) * len(slots),
        [pltpu.VMEM(ACC, f32)],
        name="merge",
    )(pos, x, other, other_lse)


def join_body(spot_ref, *refs):
    parts, o_ref = refs[:HOPS], refs[HOPS]
    for o in range(HOPS):
        head = (spot_ref[1] + o) & (HOPS - 1)
        o_ref[:, lanes_of(head)] = parts[o][...]


def join_heads(spot, parts):
    vmem = pl.BlockSpec(memory_space=pltpu.VMEM)
    return call(
        join_body,
        jax.ShapeDtypeStruct((ROWS, HOPS * HEAD), bf16),
        in_specs=[SMEM] + [vmem] * HOPS,
        name="join_heads",
    )(spot, *parts)


NEAR = [[PEERS * j + p for p in range(PEERS)] for j in range(HOPS)]
NEXT = [(PEERS * j + p, PEERS * j + (p + 1) % PEERS) for j in range(HOPS) for p in range(PEERS)]


def hop(x, o):
    count = PEERS * HOPS
    return lax.ppermute(x, "seq", [(s, (s + PEERS * o) % count) for s in range(count)])


def swap(x):
    return lax.all_to_all(x, "seq", 0, 0, tiled=True, axis_index_groups=NEAR)


def on_device(qk, values, dest_dev, dest_slot):
    return routed(qk, values, dest_dev)


def routed(qk, values, dest_dev):
    spot = jnp.stack([lax.axis_index("round"), lax.axis_index("seq") // PEERS]).astype(i32)
    other = lax.ppermute(dest_dev, "round", [(0, 1), (1, 0)])
    mine = {}
    mine[1], mine[3] = split_heads(spot, qk, values, (1, 3))
    for o in (1, 3):
        mine[o] = hop(mine[o], o)
    (mine[2],) = split_heads(spot, qk, values, (2,))
    mine[2] = hop(mine[2], 2)
    (mine[0],) = split_heads(spot, qk, values, (0,), 16 << 20)
    mine = [mine[o] for o in range(HOPS)]
    here = places(spot, dest_dev, other)
    spots = [here] + [hop(here, o) for o in range(1, HOPS)]
    sent, pos = zip(*[pack(mine, spots, r) for r in range(2)])
    got = [swap(sent[0])]
    tails = [tail_of(got[0])]
    halo = lax.ppermute(tails[0], "seq", NEXT)
    got.append(swap(sent[1]))
    reply = attend(*arranged(got[0], tails[0], halo))
    tails.append(tail_of(got[1]))
    halo = lax.ppermute(tails[1], "seq", NEXT)
    back = [swap(reply)]
    back.append(swap(attend(*arranged(got[1], tails[1], halo))))
    out, lse = unpack(pos[0], back[0])
    done = {}
    done[2], done[1] = merge(pos[1], back[1], out, lse, (2, 1))
    for o in (1, 2):
        done[o] = hop(done[o], -o)
    done[3], done[0] = merge(pos[1], back[1], out, lse, (3, 0))
    done[3] = hop(done[3], -3)
    return join_heads(spot, [done[o] for o in range(HOPS)])


def arranged(got, tail, halo):
    rows, tcol = compact(got, tail)
    return rows, halo, tcol


def solution(mesh):
    return jax.shard_map(
        on_device,
        mesh=mesh,
        in_specs=(P("seq", None), P("seq", None), P("round", "seq"), P("round", "seq")),
        out_specs=P("seq", "round"),
        check_vma=False,
    )
```
